32 devices in a mesh: section: 4 (over z), rep: 8 (over y, x, core).
Axes of the slice: x: 2, y: 2, z: 4, core: 2. Of those that a mesh axis runs over, the one named last changes fastest.
Arguments:
- cache: bfloat16 [4, 4096, 3584], P('section', 'rep'), may hold values from -6 to 6
- payload: bfloat16 [4, 4096, 3584], P('section', 'rep'), may hold values from -6 to 6
- block_ids: int32 [4, 8, 2], P('section', 'rep'), may hold values from 0 to 3, as said below
- block_counts: int32 [4, 8], P('section', 'rep'), may hold values from 1 to 2, as said below
- block_scales: int32 [4, 8, 2], P('section', 'rep'), may hold values from 1024 to 8192
- refresh_ids: int32 [4, 8, 128], P('section', 'rep'), may hold values from 0 to 511, as said below
- refresh_counts: int32 [4, 8], P('section', 'rep'), may hold values from 1 to 128, as said below
- norm_gain: float32 [4, 3584], P('section'), may hold values from 0.5 to 1.5
- query_weight: bfloat16 [4, 3584, 3584], P('section', 'rep'), may hold values from -0.09375 to 0.09375
- query_bias: float32 [4, 3584], P('section'), may hold values from -3 to 3
- kv_weight: bfloat16 [4, 3584, 1024], P('section', 'rep'), may hold values from -0.09375 to 0.09375
- kv_bias: float32 [4, 1024], P('section'), may hold values from -3 to 3
Outputs:
- rebuilt: bfloat16 [4, 4096, 3584], P('section', 'rep')
- queries: bfloat16 [4, 4096, 3584], P('section', 'rep')
- keys_values: bfloat16 [4, 4096, 1024], P('section', 'rep')
The draws below stay inside these ranges and needn't reach their ends.
Inputs may be any that keep to these rules, and one draw needn't show every extreme that they name: `block_ids`: for each section and relay the 2 entries are different block numbers; only the first block_counts entries are used. `block_counts`: in every section some relay lists exactly 2 blocks. `refresh_ids`: for each section and relay the entries are different local row numbers; only the first refresh_counts entries are used. `refresh_counts`: in every section some relay lists exactly 128 rows.
All inputs are finite; a program needn't handle non-finite values.
Results may differ from the reference program's by a relative error of at most 0.0052.
Values may be sent and summed in bfloat16 or wider, within the bound.
A program may use at most 256 MiB of HBM per device.

```python
import jax
import jax.numpy as jnp
from jax import lax

D = 3584
QW = 3584
KVW = 1024
BLK = 128
NBLK = 4
MOST_BLK = 2
REF_MAX = 128
ROW_DEV = 512
REPS = 8
SECTIONS = 4
ROWS = 4096


def pick_distinct(key, extent, amount):
    key_list = jax.random.split(key, SECTIONS * REPS)
    chosen = jax.vmap(lambda single: jax.random.permutation(single, extent)[:amount])(key_list)
    return chosen.reshape(SECTIONS, REPS, amount).astype(jnp.int32)


def counts_reaching(key, ceiling):
    front_key, place_key = jax.random.split(key)
    counts = jax.random.randint(front_key, (SECTIONS, REPS), 1, ceiling + 1)
    full_rank = jax.random.randint(place_key, (SECTIONS,), 0, REPS)
    at_full = jnp.arange(REPS)[None, :] == full_rank[:, None]
    return jnp.where(at_full, ceiling, counts).astype(jnp.int32)


def draw_block_ids(key, part):
    return pick_distinct(jax.random.fold_in(key, 11), NBLK, MOST_BLK)


def draw_block_counts(key, part):
    return counts_reaching(jax.random.fold_in(key, 12), MOST_BLK)


def draw_refresh_ids(key, part):
    return pick_distinct(jax.random.fold_in(key, 13), ROW_DEV, REF_MAX)


def draw_refresh_counts(key, part):
    return counts_reaching(jax.random.fold_in(key, 14), REF_MAX)


def touch_ends(values, own_key, low, largest):
    longest = values.shape.index(max(values.shape))
    spots = []
    for shift in (0, 1):
        where = [jax.random.randint(jax.random.fold_in(own_key, axis), (), 0, length) for axis, length in enumerate(values.shape)]
        where[longest] = (where[longest] + shift) % values.shape[longest]
        spots.append(tuple(where))
    return values.at[spots[0]].set(low).at[spots[1]].set(largest)


def level_of(stream_key, dims, pieces, smallest, largest):
    def one(axis_at, blocks):
        heights = jax.random.uniform(jax.random.fold_in(jax.random.fold_in(stream_key, 6), axis_at), (blocks,), jnp.float32, smallest / len(pieces), largest / len(pieces))
        return jnp.repeat(jnp.exp(heights), dims[axis_at] // blocks).reshape((-1,) + (1,) * (len(dims) - axis_at - 1))

    level = one(*pieces[0])
    for cut in pieces[1:]:
        level = level * one(*cut)
    return level


def scatter_about(rng, dims, deviation, bound, cuts=(), kind=jnp.bfloat16):
    entries = deviation * jax.random.normal(rng, dims, jnp.float32)
    if cuts:
        entries = entries * level_of(rng, dims, cuts, -0.22, 0.18)
    return jnp.clip(entries, -bound, bound).astype(kind)


def setup_inputs(seed: int = 0) -> dict:
    keys = jax.random.split(jax.random.key(seed), 13)
    return {
        "cache": scatter_about(keys[0], (SECTIONS, ROWS, D), 1.0, 6.0, ((0, 4), (1, 8))),
        "payload": scatter_about(keys[1], (SECTIONS, ROWS, D), 1.0, 6.0, ((0, 4), (1, 8))),
        "block_ids": draw_block_ids(jax.random.fold_in(keys[12], 71), 0),
        "block_counts": draw_block_counts(jax.random.fold_in(keys[12], 71), 0),
        "block_scales": touch_ends(jax.random.randint(keys[4], (SECTIONS, REPS, MOST_BLK), 1024, 8193), jax.random.fold_in(keys[4], 1), 1024, 8192).astype(jnp.int32),
        "refresh_ids": draw_refresh_ids(jax.random.fold_in(keys[12], 71), 0),
        "refresh_counts": draw_refresh_counts(jax.random.fold_in(keys[12], 71), 0),
        "norm_gain": jnp.clip(1.0 + 0.1 * jax.random.normal(keys[7], (SECTIONS, D), jnp.float32), 0.5, 1.5),
        "query_weight": scatter_about(keys[8], (SECTIONS, D, QW), D ** -0.5, 0.09375, ((0, 4), (1, 8))),
        "query_bias": scatter_about(keys[9], (SECTIONS, QW), 0.5, 3.0, ((0, 4),), jnp.float32),
        "kv_weight": scatter_about(keys[10], (SECTIONS, D, KVW), D ** -0.5, 0.09375, ((0, 4), (1, 8))),
        "kv_bias": scatter_about(keys[11], (SECTIONS, KVW), 0.5, 3.0, ((0, 4),), jnp.float32),
    }


def rebuild(stored, sent, ids, counts, scales, rows_sent, rows_counts):
    stored_blocks = stored.reshape(REPS, NBLK, BLK, D).astype(jnp.float32)
    sent_blocks = sent.reshape(REPS, NBLK, BLK, D).astype(jnp.float32)
    live = jnp.arange(MOST_BLK)[None, :] < counts[:, None]
    factor = jnp.where(live, scales.astype(jnp.float32) / 4096.0, 0.0)
    select = (ids[:, :, None] == jnp.arange(NBLK)[None, None, :]).astype(jnp.float32)
    per_block = lax.optimization_barrier(jnp.sum(factor[:, :, None] * select, axis=1))
    delta = (sent_blocks * per_block[:, :, None, None]).astype(jnp.bfloat16)
    delta = lax.optimization_barrier(delta).astype(jnp.float32)
    mixed = (stored_blocks + delta).reshape(REPS, ROW_DEV, D)
    live_rows = jnp.arange(REF_MAX)[None, :] < rows_counts[:, None]
    matches = (rows_sent[:, :, None] == jnp.arange(ROW_DEV)[None, None, :]) & live_rows[:, :, None]
    hit = jnp.any(matches, axis=1)
    mixed = jnp.where(hit[:, :, None], sent_blocks.reshape(REPS, ROW_DEV, D), mixed)
    return mixed.reshape(REPS * ROW_DEV, D).astype(jnp.bfloat16)

def project(rebuilt_section, gain, query_weight, query_bias, kv_weight, kv_bias):
    wide = rebuilt_section.astype(jnp.float32)
    scale_rows = lax.rsqrt(lax.optimization_barrier(jnp.mean(wide * wide, axis=1, keepdims=True)) + 1e-06)
    normed = (wide * scale_rows * gain[None, :]).astype(jnp.bfloat16)
    queries = jnp.dot(normed, query_weight, preferred_element_type=jnp.float32) + query_bias[None, :]
    keys_values = jnp.dot(normed, kv_weight, preferred_element_type=jnp.float32) + kv_bias[None, :]
    return (queries.astype(jnp.bfloat16), keys_values.astype(jnp.bfloat16))

def reference(cache, payload, block_ids, block_counts, block_scales, refresh_ids, refresh_counts, norm_gain, query_weight, query_bias, kv_weight, kv_bias):
    rebuilt_list = []
    query_list = []
    kv_list = []
    for section in range(SECTIONS):
        if section == 0:
            rebuilt_section = cache[0]
        else:
            rebuilt_section = rebuild(cache[section], payload[section - 1], block_ids[section - 1], block_counts[section - 1], block_scales[section - 1], refresh_ids[section - 1], refresh_counts[section - 1])
        queries, keys_values = project(rebuilt_section, norm_gain[section], query_weight[section], query_bias[section], kv_weight[section], kv_bias[section])
        rebuilt_list.append(rebuilt_section)
        query_list.append(queries)
        kv_list.append(keys_values)
    return (jnp.stack(rebuilt_list), jnp.stack(query_list), jnp.stack(kv_list))
```

```python
import functools

import jax
import jax.numpy as jnp
from jax import lax
from jax.experimental import pallas as pl
from jax.experimental.pallas import tpu as pltpu
from jax.sharding import PartitionSpec as P

BLK = 128
CW = 256
SLOT = 2
GW = SLOT * CW
TILE = 16
EPSILON = 1e-06
KERNEL_VMEM = 100 * 512 * 1024
OUT_VMEM = 3 * 1024 * 1024
MESH = pl.DeviceIdType.MESH


def chip_at(pos, chips):
    half = chips // 2
    back = pos // half
    return pos + back * (half + chips - 1 - 2 * pos)


def kernel(
    sections,
    reps,
    most_blk,
    lists_ref,
    payload_ref,
    cache_ref,
    gain_ref,
    qw_ref,
    qb_ref,
    kvw_ref,
    kvb_ref,
    rebuilt_ref,
    q_ref,
    kv_ref,
    last_w,
    last_normed,
    last_sums,
    w,
    normed,
    early,
    sums,
    values,
    bias,
    lists,
    local_sem,
    keep_sem,
    row_send,
    row_recv,
    own_send,
    pair_own_recv,
    ring_send,
    ring_recv,
    pair_send,
    pair_recv,
    far_send,
    far_recv,
    far_pair_send,
    far_pair_recv,
):
    chips = reps // 2
    hops = chips // 2
    depth = qw_ref.shape[1]
    rows = payload_ref.shape[1]
    feature = payload_ref.shape[2]
    ngq = qw_ref.shape[2] // GW
    ng = ngq + kvw_ref.shape[2] // GW
    nq = ngq * SLOT
    nc = ng * SLOT
    nh = nc // 2
    row_chunks = rows // BLK

    section = lax.axis_index("section")
    me = lax.axis_index("rep")
    core = me % 2
    chip = me // 2
    pos = chip + (chip // hops) * (hops + chips - 1 - 2 * chip)
    partner = 2 * chip + (1 - core)

    def rep_at(place, which):
        return 2 * chip_at((place + chips) % chips, chips) + which

    towards = (rep_at(pos + 1, core), rep_at(pos - 1, core))

    barrier = pltpu.get_barrier_semaphore()
    for other in towards + (partner,):
        pl.semaphore_signal(barrier, 1, device_id={"rep": other}, device_id_type=MESH)

    @pl.when(section > 0)
    def _():
        pl.semaphore_signal(
            barrier, 1, device_id={"section": section - 1}, device_id_type=MESH
        )

    @pl.when(section < sections - 1)
    def _():
        pl.semaphore_signal(
            barrier, 1, device_id={"section": section + 1}, device_id_type=MESH
        )

    def own(g):
        if g < ngq:
            return qw_ref.at[0, :, pl.ds(g * GW, GW)]
        return kvw_ref.at[0, :, pl.ds((g - ngq) * GW, GW)]

    def depth_of(block):
        return pl.ds(pl.multiple_of(block * depth, depth), depth)

    def columns_of(c):
        return pl.ds(pl.multiple_of((c % SLOT) * CW, CW), CW)

    def slot(g, block):
        return w.at[g, depth_of(block), :]

    def piece(c, block):
        return w.at[c // SLOT, depth_of(block), columns_of(c)]

    keep = pltpu.make_async_copy(cache_ref, rebuilt_ref, keep_sem)
    own_locals = [
        pltpu.make_async_copy(own(g), slot(g, me), local_sem.at[g]) for g in range(ng)
    ]

    sides = (section + sections - 1) // sections + (2 * sections - 2 - section) // sections
    pl.semaphore_wait(barrier, 3 + sides)

    def list_copy(i):
        return pltpu.make_async_remote_copy(
            src_ref=lists_ref[i],
            dst_ref=lists[i],
            send_sem=row_send.at[row_chunks + i],
            recv_sem=row_recv.at[row_chunks + i],
            device_id={"section": section + 1},
            device_id_type=MESH,
        )

    def row_copy(j):
        return pltpu.make_async_remote_copy(
            src_ref=payload_ref.at[0, pl.ds(j * BLK, BLK), :],
            dst_ref=values.at[pl.ds(j * BLK, BLK), :],
            send_sem=row_send.at[j],
            recv_sem=row_recv.at[j],
            device_id={"section": section + 1},
            device_id_type=MESH,
        )

    for g in range(ng):
        for d in range(2):
            pltpu.make_async_remote_copy(
                src_ref=own(g),
                dst_ref=slot(g, me),
                send_sem=own_send.at[d],
                recv_sem=ring_recv.at[d, 0, g],
                device_id={"rep": towards[d]},
                device_id_type=MESH,
            ).start()
        if g == 0:

            @pl.when(section < sections - 1)
            def _():
                for j in range(row_chunks):
                    row_copy(j).start()
                    if j == 0:
                        for i in range(len(lists)):
                            list_copy(i).start()

            keep.start()

        pltpu.make_async_remote_copy(
            src_ref=own(g),
            dst_ref=slot(g, me),
            send_sem=own_send.at[2],
            recv_sem=pair_own_recv.at[g],
            device_id={"rep": partner},
            device_id_type=MESH,
        ).start()
        own_locals[g].start()

    @pl.when(section == 0)
    def _():
        for ref in lists:
            ref[...] = jnp.zeros_like(ref)

        @pl.loop(0, rows // TILE)
        def _(i):
            values[pl.ds(i * TILE, TILE), :] = jnp.zeros((TILE, feature), values.dtype)

    for g in range(ngq):
        bias[g] = qb_ref[:, g * GW : (g + 1) * GW]
    for g in range(ngq, ng):
        bias[g] = kvb_ref[:, (g - ngq) * GW : (g - ngq + 1) * GW]
    keep.wait()
    for g in range(ng):
        own_locals[g].wait()

    def block_of(d, t, which):
        return rep_at(pos - t if d == 0 else pos + t, which)

    def landed(here, sem):
        pltpu.make_async_copy(here, here, sem).wait()

    def pass_on(here, send_sem, recv_sem, target):
        pltpu.make_async_remote_copy(
            src_ref=here,
            dst_ref=here,
            send_sem=send_sem,
            recv_sem=recv_sem,
            device_id={"rep": target},
            device_id_type=MESH,
        ).start()

    def rebuild(j):
        @pl.when(section > 0)
        def _():
            if j == 0:
                for i in range(len(lists)):
                    list_copy(i).wait_recv()
            row_copy(j).wait_recv()

        got_rows, got_ids, got_scales, got_counts, got_rcounts = lists
        count = got_counts[...]
        factor = jnp.zeros((1, 1), jnp.float32)
        for i in range(most_blk):
            live = jnp.logical_and(got_ids[:, i : i + 1] == j, count > i)
            scale = got_scales[:, i : i + 1].astype(jnp.float32) / 4096.0
            factor = factor + jnp.where(live, scale, 0.0)

        @pl.loop(0, BLK // TILE)
        def _(i):
            first = j * BLK + i * TILE
            here = pl.ds(pl.multiple_of(first, TILE), TILE)
            ids = got_rows[...]
            lanes = lax.broadcasted_iota(jnp.int32, ids.shape, 1)
            ids = jnp.where(lanes < got_rcounts[...], ids, -1)
            number = first + lax.broadcasted_iota(jnp.int32, (TILE, ids.shape[1]), 0)
            match = jnp.where(ids == number, 1.0, 0.0)
            hit = jnp.max(match, axis=1, keepdims=True) > 0.0
            got = values[here, :].astype(jnp.float32)
            delta = (got * factor).astype(jnp.bfloat16).astype(jnp.float32)
            mixed = jnp.where(hit, got, rebuilt_ref[0, here, :].astype(jnp.float32) + delta)
            rebuilt = mixed.astype(jnp.bfloat16)
            rebuilt_ref[0, here, :] = rebuilt
            wide = rebuilt.astype(jnp.float32)
            mean = jnp.sum(wide * wide, axis=1, keepdims=True) / feature
            scale_rows = lax.rsqrt(mean + EPSILON)
            result = (wide * scale_rows * gain_ref[...]).astype(jnp.bfloat16)
            for k in range(chips):
                normed[k, here, :] = result[:, 2 * depth * k : 2 * depth * (k + 1)]

    far = chip_at((pos + hops) % chips, chips)
    wide_depth = 2 * depth
    half = rows // 2

    def term(which, g, columns, first):
        rows_here = pl.ds(pl.multiple_of(which * wide_depth, wide_depth), wide_depth)
        return jnp.dot(
            normed[which, first : first + half, :],
            w[g, rows_here, columns],
            preferred_element_type=jnp.float32,
        )

    def near(g, columns, first):
        total = bias[g, :, columns]
        for step in range(1, chips):
            total = total + term((far + step) % chips, g, columns, first)
        return total

    def start(g):
        landed(slot(g, partner), pair_own_recv.at[g])
        for t in range(1, hops):
            for e in range(2):
                landed(slot(g, block_of(e, t, 1 - core)), pair_recv.at[e, t - 1, g])
        early[g] = near(g, slice(None), 0)

    marks = [(j + 1) * ng // row_chunks for j in range(row_chunks)]
    marks[-1] = ng
    ready = marks[row_chunks // 2 - 1]
    per_step = -(-ng // (ng - ready))
    for t in range(1, hops):
        done = 0
        for j, mark in enumerate(marks):

            @pl.loop(done, mark)
            def _(g):
                for d in range(2):
                    here = slot(g, block_of(d, t, core))
                    landed(here, ring_recv.at[d, t - 1, g])
                    if t + 1 < hops:
                        pass_on(here, ring_send.at[d, t - 1], ring_recv.at[d, t, g], towards[d])
                    else:
                        for k in range(SLOT):
                            c = g * SLOT + k
                            last = nh - 1 + d * nh

                            @pl.when((c < last) if d == 0 else ((c >= nh) & (c < last)))
                            def _():
                                pass_on(
                                    piece(c, block_of(d, t, core)),
                                    far_send.at[d],
                                    far_recv.at[d, c - d * nh],
                                    towards[d],
                                )

                            if k == last % SLOT:

                                @pl.when(c == last)
                                def _():
                                    pltpu.make_async_remote_copy(
                                        src_ref=w.at[
                                            last // SLOT,
                                            depth_of(block_of(d, t, core)),
                                            pl.ds(k * CW, CW),
                                        ],
                                        dst_ref=last_w.at[d, depth_of(core), :],
                                        send_sem=far_send.at[d],
                                        recv_sem=far_recv.at[d, nh - 1],
                                        device_id={"rep": towards[d]},
                                        device_id_type=MESH,
                                    ).start()

                    pass_on(here, pair_send.at[d, t - 1], pair_recv.at[d, t - 1, g], partner)
                if t + 1 == hops and (t > 1 or done >= ready):
                    for k in range(per_step):
                        other = (g - ready) * per_step + k

                        @pl.when(jnp.logical_and(other >= 0, other < ng))
                        def _():
                            start(other)

            done = mark
            if t == 1:
                rebuild(j)

    def partial(i):
        for d in range(2):
            c = i + d * nh
            sums[i % 2, d] = near(c // SLOT, columns_of(c), half)

    def paired(i):
        for d in range(2):
            c = i + d * nh
            landed(piece(c, block_of(d, hops, 1 - core)), far_pair_recv.at[d, i])

    def finish(i):
        for d in range(2):
            c = i + d * nh
            for first in (0, half):
                if first == 0:
                    total = early[c // SLOT, :, columns_of(c)]
                else:
                    total = sums[i % 2, d]
                total = total + term(far, c // SLOT, columns_of(c), first)
                result = total.astype(jnp.bfloat16)
                here = slice(first, first + half)

                @pl.when(c < nq)
                def _():
                    q_ref[0, here, pl.ds(pl.multiple_of(c * CW, CW), CW)] = result

                @pl.when(c >= nq)
                def _():
                    kv_ref[0, here, pl.ds(pl.multiple_of((c - nq) * CW, CW), CW)] = result

    def arrived(i):
        for d in range(2):
            c = i + d * nh
            here = piece(c, block_of(d, hops, core))
            landed(here, far_recv.at[d, i])
            pass_on(here, far_pair_send.at[d], far_pair_recv.at[d, i], partner)

    partial(0)
    last_normed[...] = normed[far]
    for d in range(2):
        c = nh - 1 + d * nh
        columns = slice((c % SLOT) * CW, (c % SLOT + 1) * CW)
        last_sums[d, :half, :] = early[c // SLOT, :, columns]
        last_sums[d, half:, :] = near(c // SLOT, columns, half)

    @pl.loop(0, nh - 1)
    def _(i):
        arrived(i)

        @pl.when(i + 1 < nh - 1)
        def _():
            partial(i + 1)

        paired(i)
        finish(i)

    for d in range(2):
        here = last_w.at[d, depth_of(core), :]
        landed(here, far_recv.at[d, nh - 1])
        pass_on(here, far_pair_send.at[d], far_pair_recv.at[d, nh - 1], partner)

    def sent(sem, count, width):
        part = w.at[pl.ds(0, count), pl.ds(0, depth), pl.ds(0, width)]
        pltpu.make_async_copy(part, part, sem).wait()

    for k in range(3):
        sent(own_send.at[k], ng, GW)
    for d in range(2):
        for t in range(1, hops):
            if t + 1 < hops:
                sent(ring_send.at[d, t - 1], ng, GW)
            sent(pair_send.at[d, t - 1], ng, GW)
        sent(far_send.at[d], ng, CW)

    @pl.when(section < sections - 1)
    def _():
        for i in range(len(lists)):
            list_copy(i).wait_send()
        for j in range(row_chunks):
            row_copy(j).wait_send()

    for d in range(2):
        sent(far_pair_send.at[d], ng, CW)
        landed(last_w.at[d, depth_of(1 - core), :], far_pair_recv.at[d, nh - 1])


def put_out(
    parts,
    rebuilt_ref,
    q_ref,
    kv_ref,
    last_w,
    last_normed,
    last_sums,
    rebuilt_out,
    q_out,
    kv_out,
    last,
    sem,
    last_sem,
):
    rows = q_ref.shape[1]
    nq = q_ref.shape[2] // CW
    nc = nq + kv_ref.shape[2] // CW
    last_pieces = (nc // 2 - 1, nc - 1)

    copies = []

    def out(source, target, first, stop):
        step = rows // parts
        for j in range(parts):
            here = pl.ds(j * step, step)
            columns = pl.ds(first, stop - first)
            copy = pltpu.make_async_copy(
                source.at[:, here, columns], target.at[:, here, columns], sem.at[len(copies)]
            )
            copy.start()
            copies.append(copy)

    out(rebuilt_ref, rebuilt_out, 0, rebuilt_ref.shape[2])
    for source, target, base in ((q_ref, q_out, 0), (kv_ref, kv_out, nq)):
        first = 0
        count = source.shape[2] // CW
        for c in last_pieces:
            if base <= c < base + count:
                if c - base > first:
                    out(source, target, first * CW, (c - base) * CW)
                first = c - base + 1
        if first < count:
            out(source, target, first * CW, count * CW)

    for d, c in enumerate(last_pieces):
        total = last_sums[d] + jnp.dot(
            last_normed[...], last_w[d], preferred_element_type=jnp.float32
        )
        last[d] = total.astype(jnp.bfloat16)
        target, base = (q_out, 0) if c < nq else (kv_out, nq)
        copy = pltpu.make_async_copy(
            last.at[d], target.at[0, :, pl.ds((c - base) * CW, CW)], last_sem.at[d]
        )
        copy.start()
        copies.append(copy)
    for copy in copies:
        copy.wait()


def body(
    cache,
    payload,
    block_ids,
    block_counts,
    block_scales,
    refresh_ids,
    refresh_counts,
    norm_gain,
    query_weight,
    query_bias,
    kv_weight,
    kv_bias,
):
    sections = lax.axis_size("section")
    reps = lax.axis_size("rep")
    rows, feature = cache.shape[1:]
    depth = query_weight.shape[1]
    queries = query_weight.shape[2]
    keys = kv_weight.shape[2]
    most_blk = block_ids.shape[2]
    ng = (queries + keys) // GW
    nh = ng * SLOT // 2
    hops = reps // 4
    row_chunks = rows // BLK

    lists = (refresh_ids[0], block_ids[0], block_scales[0], block_counts, refresh_counts)
    vmem = pl.BlockSpec(memory_space=pltpu.VMEM)
    anywhere = pl.BlockSpec(memory_space=pltpu.HBM)
    dma = pltpu.SemaphoreType.DMA
    results = pl.pallas_call(
        functools.partial(kernel, sections, reps, most_blk),
        out_shape=(
            pltpu.VMEM(cache.shape, cache.dtype),
            pltpu.VMEM((1, rows, queries), cache.dtype),
            pltpu.VMEM((1, rows, keys), cache.dtype),
            pltpu.VMEM((2, 2 * depth, CW), jnp.bfloat16),
            pltpu.VMEM((rows, 2 * depth), jnp.bfloat16),
            pltpu.VMEM((2, rows, CW), jnp.float32),
        ),
        in_specs=[(anywhere,) * len(lists), anywhere, anywhere, vmem, anywhere, vmem, anywhere, vmem],
        out_specs=(vmem,) * 6,
        scratch_shapes=[
            pltpu.VMEM((ng, reps * depth, GW), jnp.bfloat16),
            pltpu.VMEM((reps // 2, rows, 2 * depth), jnp.bfloat16),
            pltpu.VMEM((ng, rows // 2, GW), jnp.float32),
            pltpu.VMEM((2, 2, rows // 2, CW), jnp.float32),
            pltpu.VMEM((rows, feature), jnp.bfloat16),
            pltpu.VMEM((ng, 1, GW), jnp.float32),
            tuple(pltpu.VMEM(x.shape, x.dtype) for x in lists),
            dma((ng,)),
            dma,
            dma((row_chunks + len(lists),)),
            dma((row_chunks + len(lists),)),
            dma((3,)),
            dma((ng,)),
            dma((2, hops)),
            dma((2, hops - 1, ng)),
            dma((2, hops - 1)),
            dma((2, hops - 1, ng)),
            dma((2,)),
            dma((2, nh)),
            dma((2,)),
            dma((2, nh)),
        ],
        compiler_params=pltpu.CompilerParams(
            collective_id=0, has_side_effects=True, vmem_limit_bytes=KERNEL_VMEM
        ),
    )(lists, payload, cache, norm_gain, query_weight, query_bias, kv_weight, kv_bias)
    return tuple(
        pl.pallas_call(
            functools.partial(put_out, row_chunks),
            out_shape=tuple(pltpu.HBM(x.shape, x.dtype) for x in results[:3]),
            in_specs=[vmem] * len(results),
            out_specs=(anywhere,) * 3,
            scratch_shapes=[
                pltpu.VMEM((2, rows, CW), jnp.bfloat16),
                dma((6 * row_chunks,)),
                dma((2,)),
            ],
            compiler_params=pltpu.CompilerParams(vmem_limit_bytes=OUT_VMEM),
        )(*results)
    )


def solution(mesh):
    in_specs = (
        P("section", "rep", None),
        P("section", "rep", None),
        P("section", "rep", None),
        P("section", "rep"),
        P("section", "rep", None),
        P("section", "rep", None),
        P("section", "rep"),
        P("section", None),
        P("section", "rep", None),
        P("section", None),
        P("section", "rep", None),
        P("section", None),
    )
    out_specs = (P("section", "rep", None), P("section", "rep", None), P("section", "rep", None))
    return jax.shard_map(body, mesh=mesh, in_specs=in_specs, out_specs=out_specs, check_vma=False)
```

```python
import functools

import jax
import jax.numpy as jnp
from jax import lax
from jax.experimental import pallas as pl
from jax.experimental.pallas import tpu as pltpu
from jax.sharding import PartitionSpec as P

BLK = 128
CW = 256
SLOT = 2
GW = SLOT * CW
TILE = 16
EPSILON = 1e-06
KERNEL_VMEM = 100 * 512 * 1024
OUT_VMEM = 3 * 1024 * 1024
MESH = pl.DeviceIdType.MESH


def chip_at(pos, chips):
    half = chips // 2
    back = pos // half
    return pos + back * (half + chips - 1 - 2 * pos)


def kernel(
    sections,
    reps,
    most_blk,
    lists_ref,
    payload_ref,
    cache_ref,
    gain_hbm,
    qw_ref,
    qb_hbm,
    kvw_ref,
    kvb_hbm,
    rebuilt_ref,
    q_ref,
    kv_ref,
    last_w,
    last_normed,
    last_sums,
    w,
    normed,
    early,
    sums,
    values,
    gain_ref,
    bias,
    lists,
    local_sem,
    keep_sem,
    small_sem,
    row_send,
    row_recv,
    own_send,
    pair_own_recv,
    ring_send,
    ring_recv,
    pair_send,
    pair_recv,
    far_send,
    far_recv,
    far_pair_send,
    far_pair_recv,
):
    chips = reps // 2
    hops = chips // 2
    depth = qw_ref.shape[1]
    rows = payload_ref.shape[1]
    feature = payload_ref.shape[2]
    ngq = qw_ref.shape[2] // GW
    ng = ngq + kvw_ref.shape[2] // GW
    nq = ngq * SLOT
    nc = ng * SLOT
    nh = nc // 2
    row_chunks = rows // BLK

    section = lax.axis_index("section")
    me = lax.axis_index("rep")
    core = me % 2
    chip = me // 2
    pos = chip + (chip // hops) * (hops + chips - 1 - 2 * chip)
    partner = 2 * chip + (1 - core)

    def rep_at(place, which):
        return 2 * chip_at((place + chips) % chips, chips) + which

    towards = (rep_at(pos + 1, core), rep_at(pos - 1, core))

    barrier = pltpu.get_barrier_semaphore()
    for other in towards + (partner,):
        pl.semaphore_signal(barrier, 1, device_id={"rep": other}, device_id_type=MESH)

    @pl.when(section > 0)
    def _():
        pl.semaphore_signal(
            barrier, 1, device_id={"section": section - 1}, device_id_type=MESH
        )

    @pl.when(section < sections - 1)
    def _():
        pl.semaphore_signal(
            barrier, 1, device_id={"section": section + 1}, device_id_type=MESH
        )

    def own(g):
        if g < ngq:
            return qw_ref.at[0, :, pl.ds(g * GW, GW)]
        return kvw_ref.at[0, :, pl.ds((g - ngq) * GW, GW)]

    def depth_of(block):
        return pl.ds(pl.multiple_of(block * depth, depth), depth)

    def columns_of(c):
        return pl.ds(pl.multiple_of((c % SLOT) * CW, CW), CW)

    def slot(g, block):
        return w.at[g, depth_of(block), :]

    def piece(c, block):
        return w.at[c // SLOT, depth_of(block), columns_of(c)]

    keep = pltpu.make_async_copy(cache_ref, rebuilt_ref, keep_sem)
    small = [pltpu.make_async_copy(gain_hbm, gain_ref, small_sem.at[ng])]
    for g in range(ng):
        source, first = (qb_hbm, g) if g < ngq else (kvb_hbm, g - ngq)
        small.append(
            pltpu.make_async_copy(source.at[:, pl.ds(first * GW, GW)], bias.at[g], small_sem.at[g])
        )
    own_locals = [
        pltpu.make_async_copy(own(g), slot(g, me), local_sem.at[g]) for g in range(ng)
    ]

    sides = (section + sections - 1) // sections + (2 * sections - 2 - section) // sections
    pl.semaphore_wait(barrier, 3 + sides)

    def list_copy(i):
        return pltpu.make_async_remote_copy(
            src_ref=lists_ref[i],
            dst_ref=lists[i],
            send_sem=row_send.at[row_chunks + i],
            recv_sem=row_recv.at[row_chunks + i],
            device_id={"section": section + 1},
            device_id_type=MESH,
        )

    def row_copy(j):
        return pltpu.make_async_remote_copy(
            src_ref=payload_ref.at[0, pl.ds(j * BLK, BLK), :],
            dst_ref=values.at[pl.ds(j * BLK, BLK), :],
            send_sem=row_send.at[j],
            recv_sem=row_recv.at[j],
            device_id={"section": section + 1},
            device_id_type=MESH,
        )

    for g in range(ng):
        for d in range(2):
            pltpu.make_async_remote_copy(
                src_ref=own(g),
                dst_ref=slot(g, me),
                send_sem=own_send.at[d],
                recv_sem=ring_recv.at[d, 0, g],
                device_id={"rep": towards[d]},
                device_id_type=MESH,
            ).start()
        if g == 0:

            @pl.when(section < sections - 1)
            def _():
                for j in range(row_chunks):
                    row_copy(j).start()
                    if j == 0:
                        for i in range(len(lists)):
                            list_copy(i).start()

            keep.start()
            for copy in small:
                copy.start()

        pltpu.make_async_remote_copy(
            src_ref=own(g),
            dst_ref=slot(g, me),
            send_sem=own_send.at[2],
            recv_sem=pair_own_recv.at[g],
            device_id={"rep": partner},
            device_id_type=MESH,
        ).start()
        own_locals[g].start()

    @pl.when(section == 0)
    def _():
        for ref in lists:
            ref[...] = jnp.zeros_like(ref)

        @pl.loop(0, rows // TILE)
        def _(i):
            values[pl.ds(i * TILE, TILE), :] = jnp.zeros((TILE, feature), values.dtype)

    for copy in small:
        copy.wait()
    keep.wait()
    for g in range(ng):
        own_locals[g].wait()

    def block_of(d, t, which):
        return rep_at(pos - t if d == 0 else pos + t, which)

    def landed(here, sem):
        pltpu.make_async_copy(here, here, sem).wait()

    def pass_on(here, send_sem, recv_sem, target):
        pltpu.make_async_remote_copy(
            src_ref=here,
            dst_ref=here,
            send_sem=send_sem,
            recv_sem=recv_sem,
            device_id={"rep": target},
            device_id_type=MESH,
        ).start()

    def rebuild(j):
        @pl.when(section > 0)
        def _():
            if j == 0:
                for i in range(len(lists)):
                    list_copy(i).wait_recv()
            row_copy(j).wait_recv()

        got_rows, got_ids, got_scales, got_counts, got_rcounts = lists
        count = got_counts[...]
        factor = jnp.zeros((1, 1), jnp.float32)
        for i in range(most_blk):
            live = jnp.logical_and(got_ids[:, i : i + 1] == j, count > i)
            scale = got_scales[:, i : i + 1].astype(jnp.float32) / 4096.0
            factor = factor + jnp.where(live, scale, 0.0)

        @pl.loop(0, BLK // TILE)
        def _(i):
            first = j * BLK + i * TILE
            here = pl.ds(pl.multiple_of(first, TILE), TILE)
            ids = got_rows[...]
            lanes = lax.broadcasted_iota(jnp.int32, ids.shape, 1)
            ids = jnp.where(lanes < got_rcounts[...], ids, -1)
            number = first + lax.broadcasted_iota(jnp.int32, (TILE, ids.shape[1]), 0)
            match = jnp.where(ids == number, 1.0, 0.0)
            hit = jnp.max(match, axis=1, keepdims=True) > 0.0
            got = values[here, :].astype(jnp.float32)
            delta = (got * factor).astype(jnp.bfloat16).astype(jnp.float32)
            mixed = jnp.where(hit, got, rebuilt_ref[0, here, :].astype(jnp.float32) + delta)
            rebuilt = mixed.astype(jnp.bfloat16)
            rebuilt_ref[0, here, :] = rebuilt
            wide = rebuilt.astype(jnp.float32)
            mean = jnp.sum(wide * wide, axis=1, keepdims=True) / feature
            scale_rows = lax.rsqrt(mean + EPSILON)
            result = (wide * scale_rows * gain_ref[...]).astype(jnp.bfloat16)
            for k in range(chips):
                normed[k, here, :] = result[:, 2 * depth * k : 2 * depth * (k + 1)]

    far = chip_at((pos + hops) % chips, chips)
    wide_depth = 2 * depth
    half = rows // 2

    def term(which, g, columns, first):
        rows_here = pl.ds(pl.multiple_of(which * wide_depth, wide_depth), wide_depth)
        return jnp.dot(
            normed[which, first : first + half, :],
            w[g, rows_here, columns],
            preferred_element_type=jnp.float32,
        )

    def near(g, columns, first):
        total = bias[g, :, columns]
        for step in range(1, chips):
            total = total + term((far + step) % chips, g, columns, first)
        return total

    def start(g):
        landed(slot(g, partner), pair_own_recv.at[g])
        for t in range(1, hops):
            for e in range(2):
                landed(slot(g, block_of(e, t, 1 - core)), pair_recv.at[e, t - 1, g])
        early[g] = near(g, slice(None), 0)

    marks = [(j + 1) * ng // row_chunks for j in range(row_chunks)]
    marks[-1] = ng
    ready = marks[row_chunks // 2 - 1]
    per_step = -(-ng // (ng - ready))
    for t in range(1, hops):
        done = 0
        for j, mark in enumerate(marks):

            @pl.loop(done, mark)
            def _(g):
                for d in range(2):
                    here = slot(g, block_of(d, t, core))
                    landed(here, ring_recv.at[d, t - 1, g])
                    if t + 1 < hops:
                        pass_on(here, ring_send.at[d, t - 1], ring_recv.at[d, t, g], towards[d])
                    else:
                        for k in range(SLOT):
                            c = g * SLOT + k
                            last = nh - 1 + d * nh

                            @pl.when((c < last) if d == 0 else ((c >= nh) & (c < last)))
                            def _():
                                pass_on(
                                    piece(c, block_of(d, t, core)),
                                    far_send.at[d],
                                    far_recv.at[d, c - d * nh],
                                    towards[d],
                                )

                            if k == last % SLOT:

                                @pl.when(c == last)
                                def _():
                                    pltpu.make_async_remote_copy(
                                        src_ref=w.at[
                                            last // SLOT,
                                            depth_of(block_of(d, t, core)),
                                            pl.ds(k * CW, CW),
                                        ],
                                        dst_ref=last_w.at[d, depth_of(core), :],
                                        send_sem=far_send.at[d],
                                        recv_sem=far_recv.at[d, nh - 1],
                                        device_id={"rep": towards[d]},
                                        device_id_type=MESH,
                                    ).start()

                    pass_on(here, pair_send.at[d, t - 1], pair_recv.at[d, t - 1, g], partner)
                if t + 1 == hops and (t > 1 or done >= ready):
                    for k in range(per_step):
                        other = (g - ready) * per_step + k

                        @pl.when(jnp.logical_and(other >= 0, other < ng))
                        def _():
                            start(other)

            done = mark
            if t == 1:
                rebuild(j)

    def partial(i):
        for d in range(2):
            c = i + d * nh
            sums[i % 2, d] = near(c // SLOT, columns_of(c), half)

    def paired(i):
        for d in range(2):
            c = i + d * nh
            landed(piece(c, block_of(d, hops, 1 - core)), far_pair_recv.at[d, i])

    def finish(i):
        for d in range(2):
            c = i + d * nh
            for first in (0, half):
                if first == 0:
                    total = early[c // SLOT, :, columns_of(c)]
                else:
                    total = sums[i % 2, d]
                total = total + term(far, c // SLOT, columns_of(c), first)
                result = total.astype(jnp.bfloat16)
                here = slice(first, first + half)

                @pl.when(c < nq)
                def _():
                    q_ref[0, here, pl.ds(pl.multiple_of(c * CW, CW), CW)] = result

                @pl.when(c >= nq)
                def _():
                    kv_ref[0, here, pl.ds(pl.multiple_of((c - nq) * CW, CW), CW)] = result

    def arrived(i):
        for d in range(2):
            c = i + d * nh
            here = piece(c, block_of(d, hops, core))
            landed(here, far_recv.at[d, i])
            pass_on(here, far_pair_send.at[d], far_pair_recv.at[d, i], partner)

    partial(0)
    last_normed[...] = normed[far]
    for d in range(2):
        c = nh - 1 + d * nh
        columns = slice((c % SLOT) * CW, (c % SLOT + 1) * CW)
        last_sums[d, :half, :] = early[c // SLOT, :, columns]
        last_sums[d, half:, :] = near(c // SLOT, columns, half)

    @pl.loop(0, nh - 1)
    def _(i):
        arrived(i)

        @pl.when(i + 1 < nh - 1)
        def _():
            partial(i + 1)

        paired(i)
        finish(i)

    for d in range(2):
        here = last_w.at[d, depth_of(core), :]
        landed(here, far_recv.at[d, nh - 1])
        pass_on(here, far_pair_send.at[d], far_pair_recv.at[d, nh - 1], partner)

    def sent(sem, count, width):
        part = w.at[pl.ds(0, count), pl.ds(0, depth), pl.ds(0, width)]
        pltpu.make_async_copy(part, part, sem).wait()

    for k in range(3):
        sent(own_send.at[k], ng, GW)
    for d in range(2):
        for t in range(1, hops):
            if t + 1 < hops:
                sent(ring_send.at[d, t - 1], ng, GW)
            sent(pair_send.at[d, t - 1], ng, GW)
        sent(far_send.at[d], ng, CW)

    @pl.when(section < sections - 1)
    def _():
        for i in range(len(lists)):
            list_copy(i).wait_send()
        for j in range(row_chunks):
            row_copy(j).wait_send()

    for d in range(2):
        sent(far_pair_send.at[d], ng, CW)
        landed(last_w.at[d, depth_of(1 - core), :], far_pair_recv.at[d, nh - 1])


def put_out(
    parts,
    rebuilt_ref,
    q_ref,
    kv_ref,
    last_w,
    last_normed,
    last_sums,
    rebuilt_out,
    q_out,
    kv_out,
    last,
    sem,
    last_sem,
):
    rows = q_ref.shape[1]
    nq = q_ref.shape[2] // CW
    nc = nq + kv_ref.shape[2] // CW
    last_pieces = (nc // 2 - 1, nc - 1)

    copies = []

    def out(source, target, first, stop):
        step = rows // parts
        for j in range(parts):
            here = pl.ds(j * step, step)
            columns = pl.ds(first, stop - first)
            copy = pltpu.make_async_copy(
                source.at[:, here, columns], target.at[:, here, columns], sem.at[len(copies)]
            )
            copy.start()
            copies.append(copy)

    out(rebuilt_ref, rebuilt_out, 0, rebuilt_ref.shape[2])
    for source, target, base in ((q_ref, q_out, 0), (kv_ref, kv_out, nq)):
        first = 0
        count = source.shape[2] // CW
        for c in last_pieces:
            if base <= c < base + count:
                if c - base > first:
                    out(source, target, first * CW, (c - base) * CW)
                first = c - base + 1
        if first < count:
            out(source, target, first * CW, count * CW)

    for d, c in enumerate(last_pieces):
        total = last_sums[d] + jnp.dot(
            last_normed[...], last_w[d], preferred_element_type=jnp.float32
        )
        last[d] = total.astype(jnp.bfloat16)
        target, base = (q_out, 0) if c < nq else (kv_out, nq)
        copy = pltpu.make_async_copy(
            last.at[d], target.at[0, :, pl.ds((c - base) * CW, CW)], last_sem.at[d]
        )
        copy.start()
        copies.append(copy)
    for copy in copies:
        copy.wait()


def body(
    cache,
    payload,
    block_ids,
    block_counts,
    block_scales,
    refresh_ids,
    refresh_counts,
    norm_gain,
    query_weight,
    query_bias,
    kv_weight,
    kv_bias,
):
    sections = lax.axis_size("section")
    reps = lax.axis_size("rep")
    rows, feature = cache.shape[1:]
    depth = query_weight.shape[1]
    queries = query_weight.shape[2]
    keys = kv_weight.shape[2]
    most_blk = block_ids.shape[2]
    ng = (queries + keys) // GW
    nh = ng * SLOT // 2
    hops = reps // 4
    row_chunks = rows // BLK

    lists = (refresh_ids[0], block_ids[0], block_scales[0], block_counts, refresh_counts)
    vmem = pl.BlockSpec(memory_space=pltpu.VMEM)
    anywhere = pl.BlockSpec(memory_space=pltpu.HBM)
    dma = pltpu.SemaphoreType.DMA
    results = pl.pallas_call(
        functools.partial(kernel, sections, reps, most_blk),
        out_shape=(
            pltpu.VMEM(cache.shape, cache.dtype),
            pltpu.VMEM((1, rows, queries), cache.dtype),
            pltpu.VMEM((1, rows, keys), cache.dtype),
            pltpu.VMEM((2, 2 * depth, CW), jnp.bfloat16),
            pltpu.VMEM((rows, 2 * depth), jnp.bfloat16),
            pltpu.VMEM((2, rows, CW), jnp.float32),
        ),
        in_specs=[(anywhere,) * len(lists)] + [anywhere] * 7,
        out_specs=(vmem,) * 6,
        scratch_shapes=[
            pltpu.VMEM((ng, reps * depth, GW), jnp.bfloat16),
            pltpu.VMEM((reps // 2, rows, 2 * depth), jnp.bfloat16),
            pltpu.VMEM((ng, rows // 2, GW), jnp.float32),
            pltpu.VMEM((2, 2, rows // 2, CW), jnp.float32),
            pltpu.VMEM((rows, feature), jnp.bfloat16),
            pltpu.VMEM(norm_gain.shape, jnp.float32),
            pltpu.VMEM((ng, 1, GW), jnp.float32),
            tuple(pltpu.VMEM(x.shape, x.dtype) for x in lists),
            dma((ng,)),
            dma,
            dma((ng + 1,)),
            dma((row_chunks + len(lists),)),
            dma((row_chunks + len(lists),)),
            dma((3,)),
            dma((ng,)),
            dma((2, hops)),
            dma((2, hops - 1, ng)),
            dma((2, hops - 1)),
            dma((2, hops - 1, ng)),
            dma((2,)),
            dma((2, nh)),
            dma((2,)),
            dma((2, nh)),
        ],
        compiler_params=pltpu.CompilerParams(
            collective_id=0, has_side_effects=True, vmem_limit_bytes=KERNEL_VMEM
        ),
    )(lists, payload, cache, norm_gain, query_weight, query_bias, kv_weight, kv_bias)
    return tuple(
        pl.pallas_call(
            functools.partial(put_out, 2),
            out_shape=tuple(pltpu.HBM(x.shape, x.dtype) for x in results[:3]),
            in_specs=[vmem] * len(results),
            out_specs=(anywhere,) * 3,
            scratch_shapes=[
                pltpu.VMEM((2, rows, CW), jnp.bfloat16),
                dma((6 * 2,)),
                dma((2,)),
            ],
            compiler_params=pltpu.CompilerParams(vmem_limit_bytes=OUT_VMEM),
        )(*results)
    )


def solution(mesh):
    in_specs = (
        P("section", "rep", None),
        P("section", "rep", None),
        P("section", "rep", None),
        P("section", "rep"),
        P("section", "rep", None),
        P("section", "rep", None),
        P("section", "rep"),
        P("section", None),
        P("section", "rep", None),
        P("section", None),
        P("section", "rep", None),
        P("section", None),
    )
    out_specs = (P("section", "rep", None), P("section", "rep", None), P("section", "rep", None))
    return jax.shard_map(body, mesh=mesh, in_specs=in_specs, out_specs=out_specs, check_vma=False)
```

```python
import functools

import jax
import jax.numpy as jnp
from jax import lax
from jax.experimental import pallas as pl
from jax.experimental.pallas import tpu as pltpu
from jax.sharding import PartitionSpec as P

BLK = 128
CW = 256
SLOT = 2
GW = SLOT * CW
TILE = 16
EPSILON = 1e-06
KERNEL_VMEM = 100 * 512 * 1024
OUT_VMEM = 3 * 1024 * 1024
MESH = pl.DeviceIdType.MESH


def chip_at(pos, chips):
    half = chips // 2
    back = pos // half
    return pos + back * (half + chips - 1 - 2 * pos)


def kernel(
    sections,
    reps,
    most_blk,
    lists_ref,
    payload_ref,
    cache_ref,
    gain_hbm,
    qw_ref,
    qb_hbm,
    kvw_ref,
    kvb_hbm,
    rebuilt_ref,
    q_ref,
    kv_ref,
    last_w,
    last_normed,
    last_sums,
    w,
    normed,
    early,
    sums,
    values,
    gain_ref,
    bias,
    lists,
    local_sem,
    keep_sem,
    small_sem,
    row_send,
    row_recv,
    list_send,
    list_recv,
    own_send,
    pass_send,
    ring_recv,
    pair_recv,
    far_recv,
    far_pair_recv,
):
    chips = reps // 2
    hops = chips // 2
    depth = qw_ref.shape[1]
    rows = payload_ref.shape[1]
    feature = payload_ref.shape[2]
    ngq = qw_ref.shape[2] // GW
    ng = ngq + kvw_ref.shape[2] // GW
    nq = ngq * SLOT
    nc = ng * SLOT
    nh = nc // 2
    row_chunks = rows // BLK

    section = lax.axis_index("section")
    me = lax.axis_index("rep")
    core = me % 2
    chip = me // 2
    pos = chip + (chip // hops) * (hops + chips - 1 - 2 * chip)
    partner = 2 * chip + (1 - core)

    def rep_at(place, which):
        return 2 * chip_at((place + chips) % chips, chips) + which

    towards = (rep_at(pos + 1, core), rep_at(pos - 1, core))

    barrier = pltpu.get_barrier_semaphore()
    for other in towards + (partner,):
        pl.semaphore_signal(barrier, 1, device_id={"rep": other}, device_id_type=MESH)

    @pl.when(section > 0)
    def _():
        pl.semaphore_signal(
            barrier, 1, device_id={"section": section - 1}, device_id_type=MESH
        )

    @pl.when(section < sections - 1)
    def _():
        pl.semaphore_signal(
            barrier, 1, device_id={"section": section + 1}, device_id_type=MESH
        )

    def own(g):
        if g < ngq:
            return qw_ref.at[0, :, pl.ds(g * GW, GW)]
        return kvw_ref.at[0, :, pl.ds((g - ngq) * GW, GW)]

    def depth_of(block):
        return pl.ds(pl.multiple_of(block * depth, depth), depth)

    def columns_of(c):
        return pl.ds(pl.multiple_of((c % SLOT) * CW, CW), CW)

    def slot(g, block):
        return w.at[g, depth_of(block), :]

    def piece(c, block):
        return w.at[c // SLOT, depth_of(block), columns_of(c)]

    keep = pltpu.make_async_copy(cache_ref, rebuilt_ref, keep_sem)
    gain_copy = pltpu.make_async_copy(gain_hbm, gain_ref, small_sem.at[0])
    small = [gain_copy]
    for g in range(ng):
        source, first = (qb_hbm, g) if g < ngq else (kvb_hbm, g - ngq)
        small.append(
            pltpu.make_async_copy(source.at[:, pl.ds(first * GW, GW)], bias.at[g], small_sem.at[1])
        )
    own_locals = [
        pltpu.make_async_copy(own(g), slot(g, me), local_sem) for g in range(ng)
    ]

    sides = (section + sections - 1) // sections + (2 * sections - 2 - section) // sections
    pl.semaphore_wait(barrier, 3 + sides)

    def list_copy(i):
        return pltpu.make_async_remote_copy(
            src_ref=lists_ref[i],
            dst_ref=lists[i],
            send_sem=list_send.at[i],
            recv_sem=list_recv.at[i],
            device_id={"section": section + 1},
            device_id_type=MESH,
        )

    def row_copy(j):
        return pltpu.make_async_remote_copy(
            src_ref=payload_ref.at[0, pl.ds(j * BLK, BLK), :],
            dst_ref=values.at[pl.ds(j * BLK, BLK), :],
            send_sem=row_send,
            recv_sem=row_recv.at[j],
            device_id={"section": section + 1},
            device_id_type=MESH,
        )

    for g in range(ng):
        for d in range(2):
            pltpu.make_async_remote_copy(
                src_ref=own(g),
                dst_ref=slot(g, me),
                send_sem=own_send,
                recv_sem=ring_recv.at[0, g],
                device_id={"rep": towards[d]},
                device_id_type=MESH,
            ).start()
        if g == 0:

            @pl.when(section < sections - 1)
            def _():
                for j in range(row_chunks):
                    row_copy(j).start()
                    if j == 0:
                        for i in range(len(lists)):
                            list_copy(i).start()

            keep.start()
            for copy in small:
                copy.start()

        pltpu.make_async_remote_copy(
            src_ref=own(g),
            dst_ref=slot(g, me),
            send_sem=own_send,
            recv_sem=pair_recv.at[g],
            device_id={"rep": partner},
            device_id_type=MESH,
        ).start()
        own_locals[g].start()

    @pl.when(section == 0)
    def _():
        for ref in lists:
            ref[...] = jnp.zeros_like(ref)

        @pl.loop(0, rows // TILE)
        def _(i):
            values[pl.ds(i * TILE, TILE), :] = jnp.zeros((TILE, feature), values.dtype)

    def landed(sem, blocks, width=GW, slots=1):
        part = w.at[pl.ds(0, slots), pl.ds(0, blocks * depth), pl.ds(0, width)]
        pltpu.make_async_copy(part, part, sem).wait()

    gain_copy.wait()
    pltpu.make_async_copy(bias, bias, small_sem.at[1]).wait()
    keep.wait()
    landed(local_sem, 1, slots=ng)

    def block_of(d, t, which):
        return rep_at(pos - t if d == 0 else pos + t, which)

    def pass_on(here, recv_sem, target):
        pltpu.make_async_remote_copy(
            src_ref=here,
            dst_ref=here,
            send_sem=pass_send,
            recv_sem=recv_sem,
            device_id={"rep": target},
            device_id_type=MESH,
        ).start()

    def rebuild(j):
        @pl.when(section > 0)
        def _():
            if j == 0:
                for i in range(len(lists)):
                    list_copy(i).wait_recv()
            row_copy(j).wait_recv()

        got_rows, got_ids, got_scales, got_counts, got_rcounts = lists
        count = got_counts[...]
        factor = jnp.zeros((1, 1), jnp.float32)
        for i in range(most_blk):
            live = jnp.logical_and(got_ids[:, i : i + 1] == j, count > i)
            scale = got_scales[:, i : i + 1].astype(jnp.float32) / 4096.0
            factor = factor + jnp.where(live, scale, 0.0)

        @pl.loop(0, BLK // TILE)
        def _(i):
            first = j * BLK + i * TILE
            here = pl.ds(pl.multiple_of(first, TILE), TILE)
            ids = got_rows[...]
            lanes = lax.broadcasted_iota(jnp.int32, ids.shape, 1)
            ids = jnp.where(lanes < got_rcounts[...], ids, -1)
            number = first + lax.broadcasted_iota(jnp.int32, (TILE, ids.shape[1]), 0)
            match = jnp.where(ids == number, 1.0, 0.0)
            hit = jnp.max(match, axis=1, keepdims=True) > 0.0
            got = values[here, :].astype(jnp.float32)
            delta = (got * factor).astype(jnp.bfloat16).astype(jnp.float32)
            mixed = jnp.where(hit, got, rebuilt_ref[0, here, :].astype(jnp.float32) + delta)
            rebuilt = mixed.astype(jnp.bfloat16)
            rebuilt_ref[0, here, :] = rebuilt
            wide = rebuilt.astype(jnp.float32)
            mean = jnp.sum(wide * wide, axis=1, keepdims=True) / feature
            scale_rows = lax.rsqrt(mean + EPSILON)
            result = (wide * scale_rows * gain_ref[...]).astype(jnp.bfloat16)
            for k in range(chips):
                normed[k, here, :] = result[:, 2 * depth * k : 2 * depth * (k + 1)]

    far = chip_at((pos + hops) % chips, chips)
    wide_depth = 2 * depth
    half = rows // 2

    def term(which, g, columns, first):
        rows_here = pl.ds(pl.multiple_of(which * wide_depth, wide_depth), wide_depth)
        return jnp.dot(
            normed[which, first : first + half, :],
            w[g, rows_here, columns],
            preferred_element_type=jnp.float32,
        )

    def near(g, columns, first):
        total = bias[g, :, columns]
        for step in range(1, chips):
            total = total + term((far + step) % chips, g, columns, first)
        return total

    def start(g):
        landed(pair_recv.at[g], 2 * hops - 1)
        early[g] = near(g, slice(None), 0)

    marks = [(j + 1) * ng // row_chunks for j in range(row_chunks)]
    marks[-1] = ng
    ready = marks[row_chunks // 2 - 1]
    per_step = -(-ng // (ng - ready))
    for t in range(1, hops):
        done = 0
        for j, mark in enumerate(marks):

            @pl.loop(done, mark)
            def _(g):
                landed(ring_recv.at[t - 1, g], 2)
                for d in range(2):
                    here = slot(g, block_of(d, t, core))
                    if t + 1 < hops:
                        pass_on(here, ring_recv.at[t, g], towards[d])
                    else:
                        for k in range(SLOT):
                            c = g * SLOT + k
                            last = nh - 1 + d * nh

                            @pl.when((c < last) if d == 0 else ((c >= nh) & (c < last)))
                            def _():
                                pass_on(
                                    piece(c, block_of(d, t, core)),
                                    far_recv.at[c - d * nh],
                                    towards[d],
                                )

                            if k == last % SLOT:

                                @pl.when(c == last)
                                def _():
                                    pltpu.make_async_remote_copy(
                                        src_ref=w.at[
                                            last // SLOT,
                                            depth_of(block_of(d, t, core)),
                                            pl.ds(k * CW, CW),
                                        ],
                                        dst_ref=last_w.at[d, depth_of(core), :],
                                        send_sem=pass_send,
                                        recv_sem=far_recv.at[nh - 1],
                                        device_id={"rep": towards[d]},
                                        device_id_type=MESH,
                                    ).start()

                    pass_on(here, pair_recv.at[g], partner)
                if t + 1 == hops and (t > 1 or done >= ready):
                    for k in range(per_step):
                        other = (g - ready) * per_step + k

                        @pl.when(jnp.logical_and(other >= 0, other < ng))
                        def _():
                            start(other)

            done = mark
            if t == 1:
                rebuild(j)

    def partial(i):
        for d in range(2):
            c = i + d * nh
            sums[i % 2, d] = near(c // SLOT, columns_of(c), half)

    def finish(i):
        for d in range(2):
            c = i + d * nh
            for first in (0, half):
                if first == 0:
                    total = early[c // SLOT, :, columns_of(c)]
                else:
                    total = sums[i % 2, d]
                total = total + term(far, c // SLOT, columns_of(c), first)
                result = total.astype(jnp.bfloat16)
                here = slice(first, first + half)

                @pl.when(c < nq)
                def _():
                    q_ref[0, here, pl.ds(pl.multiple_of(c * CW, CW), CW)] = result

                @pl.when(c >= nq)
                def _():
                    kv_ref[0, here, pl.ds(pl.multiple_of((c - nq) * CW, CW), CW)] = result

    def arrived(i):
        landed(far_recv.at[i], 2, CW)
        for d in range(2):
            pass_on(piece(i + d * nh, block_of(d, hops, core)), far_pair_recv.at[i], partner)

    partial(0)
    last_normed[...] = normed[far]
    for d in range(2):
        c = nh - 1 + d * nh
        columns = slice((c % SLOT) * CW, (c % SLOT + 1) * CW)
        last_sums[d, :half, :] = early[c // SLOT, :, columns]
        last_sums[d, half:, :] = near(c // SLOT, columns, half)

    @pl.loop(0, nh - 1)
    def _(i):
        arrived(i)

        @pl.when(i + 1 < nh - 1)
        def _():
            partial(i + 1)

        landed(far_pair_recv.at[i], 2, CW)
        finish(i)

    landed(far_recv.at[nh - 1], 2, CW)
    for d in range(2):
        pass_on(last_w.at[d, depth_of(core), :], far_pair_recv.at[nh - 1], partner)

    landed(own_send, 3, slots=ng)

    @pl.when(section < sections - 1)
    def _():
        for i in range(len(lists)):
            list_copy(i).wait_send()
        pltpu.make_async_copy(values, values, row_send).wait()

    landed(pass_send, 4 * hops - 4, slots=ng)
    landed(far_pair_recv.at[nh - 1], 2, CW)


def put_out(
    parts,
    rebuilt_ref,
    q_ref,
    kv_ref,
    last_w,
    last_normed,
    last_sums,
    rebuilt_out,
    q_out,
    kv_out,
    last,
    sem,
):
    rows = q_ref.shape[1]
    nq = q_ref.shape[2] // CW
    nc = nq + kv_ref.shape[2] // CW
    last_pieces = (nc // 2 - 1, nc - 1)

    step = rows // parts

    def out(source, target, base, k):
        count = source.shape[2] // CW
        cuts = [c - base for c in last_pieces if base <= c < base + count]
        for first, stop in zip([0] + [c + 1 for c in cuts], cuts + [count]):
            if first < stop:
                columns = pl.ds(first * CW, (stop - first) * CW)
                for j in range(parts):
                    here = pl.ds(j * step, step)
                    pltpu.make_async_copy(
                        source.at[:, here, columns], target.at[:, here, columns], sem.at[k]
                    ).start()
        whole = source.at[:, :, pl.ds(0, (count - len(cuts)) * CW)]
        return pltpu.make_async_copy(whole, whole, sem.at[k])

    arrays = ((rebuilt_ref, rebuilt_out, nc), (q_ref, q_out, 0), (kv_ref, kv_out, nq))
    waits = [out(source, target, base, k) for k, (source, target, base) in enumerate(arrays)]
    for d, c in enumerate(last_pieces):
        total = last_sums[d] + jnp.dot(
            last_normed[...], last_w[d], preferred_element_type=jnp.float32
        )
        last[d] = total.astype(jnp.bfloat16)
        target, base = (q_out, 0) if c < nq else (kv_out, nq)
        pltpu.make_async_copy(
            last.at[d], target.at[0, :, pl.ds((c - base) * CW, CW)], sem.at[len(arrays)]
        ).start()
    for copy in waits:
        copy.wait()
    pltpu.make_async_copy(last, last, sem.at[len(arrays)]).wait()


def body(
    cache,
    payload,
    block_ids,
    block_counts,
    block_scales,
    refresh_ids,
    refresh_counts,
    norm_gain,
    query_weight,
    query_bias,
    kv_weight,
    kv_bias,
):
    sections = lax.axis_size("section")
    reps = lax.axis_size("rep")
    rows, feature = cache.shape[1:]
    depth = query_weight.shape[1]
    queries = query_weight.shape[2]
    keys = kv_weight.shape[2]
    most_blk = block_ids.shape[2]
    ng = (queries + keys) // GW
    nh = ng * SLOT // 2
    hops = reps // 4
    row_chunks = rows // BLK

    lists = (refresh_ids[0], block_ids[0], block_scales[0], block_counts, refresh_counts)
    vmem = pl.BlockSpec(memory_space=pltpu.VMEM)
    anywhere = pl.BlockSpec(memory_space=pltpu.HBM)
    dma = pltpu.SemaphoreType.DMA
    results = pl.pallas_call(
        functools.partial(kernel, sections, reps, most_blk),
        out_shape=(
            pltpu.VMEM(cache.shape, cache.dtype),
            pltpu.VMEM((1, rows, queries), cache.dtype),
            pltpu.VMEM((1, rows, keys), cache.dtype),
            pltpu.VMEM((2, 2 * depth, CW), jnp.bfloat16),
            pltpu.VMEM((rows, 2 * depth), jnp.bfloat16),
            pltpu.VMEM((2, rows, CW), jnp.float32),
        ),
        in_specs=[(anywhere,) * len(lists)] + [anywhere] * 7,
        out_specs=(vmem,) * 6,
        scratch_shapes=[
            pltpu.VMEM((ng, reps * depth, GW), jnp.bfloat16),
            pltpu.VMEM((reps // 2, rows, 2 * depth), jnp.bfloat16),
            pltpu.VMEM((ng, rows // 2, GW), jnp.float32),
            pltpu.VMEM((2, 2, rows // 2, CW), jnp.float32),
            pltpu.VMEM((rows, feature), jnp.bfloat16),
            pltpu.VMEM(norm_gain.shape, jnp.float32),
            pltpu.VMEM((ng, 1, GW), jnp.float32),
            tuple(pltpu.VMEM(x.shape, x.dtype) for x in lists),
            dma,
            dma,
            dma((2,)),
            dma,
            dma((row_chunks,)),
            dma((len(lists),)),
            dma((len(lists),)),
            dma,
            dma,
            dma((hops - 1, ng)),
            dma((ng,)),
            dma((nh,)),
            dma((nh,)),
        ],
        compiler_params=pltpu.CompilerParams(
            collective_id=0, has_side_effects=True, vmem_limit_bytes=KERNEL_VMEM
        ),
    )(lists, payload, cache, norm_gain, query_weight, query_bias, kv_weight, kv_bias)
    return tuple(
        pl.pallas_call(
            functools.partial(put_out, 2),
            out_shape=tuple(pltpu.HBM(x.shape, x.dtype) for x in results[:3]),
            in_specs=[vmem] * len(results),
            out_specs=(anywhere,) * 3,
            scratch_shapes=[
                pltpu.VMEM((2, rows, CW), jnp.bfloat16),
                dma((4,)),
            ],
            compiler_params=pltpu.CompilerParams(vmem_limit_bytes=OUT_VMEM),
        )(*results)
    )


def solution(mesh):
    in_specs = (
        P("section", "rep", None),
        P("section", "rep", None),
        P("section", "rep", None),
        P("section", "rep"),
        P("section", "rep", None),
        P("section", "rep", None),
        P("section", "rep"),
        P("section", None),
        P("section", "rep", None),
        P("section", None),
        P("section", "rep", None),
        P("section", None),
    )
    out_specs = (P("section", "rep", None), P("section", "rep", None), P("section", "rep", None))
    return jax.shard_map(body, mesh=mesh, in_specs=in_specs, out_specs=out_specs, check_vma=False)
```

```python
import functools

import jax
import jax.numpy as jnp
from jax import lax
from jax.experimental import pallas as pl
from jax.experimental.pallas import tpu as pltpu
from jax.sharding import PartitionSpec as P

BLK = 128
HALF = 128
CW = 256
SLOT = 2
GW = SLOT * CW
TILE = 16
EPSILON = 1e-06
KERNEL_VMEM = 100 * 512 * 1024
OUT_VMEM = 3 * 1024 * 1024
MESH = pl.DeviceIdType.MESH


def chip_at(pos, chips):
    half = chips // 2
    back = pos // half
    return pos + back * (half + chips - 1 - 2 * pos)


def kernel(
    sections,
    reps,
    most_blk,
    lists_ref,
    payload_ref,
    cache_ref,
    gain_hbm,
    qw_ref,
    qb_hbm,
    kvw_ref,
    kvb_hbm,
    rebuilt_ref,
    q_ref,
    kv_ref,
    last_w,
    last_normed,
    last_sums,
    w,
    normed,
    early,
    sums,
    values,
    gain_ref,
    bias,
    lists,
    local_sem,
    keep_sem,
    small_sem,
    row_send,
    row_recv,
    list_send,
    list_recv,
    own_send,
    pass_send,
    ring_recv,
    pair_recv,
    far_recv,
    far_pair_recv,
):
    chips = reps // 2
    hops = chips // 2
    depth = qw_ref.shape[1]
    rows = payload_ref.shape[1]
    feature = payload_ref.shape[2]
    ngq = qw_ref.shape[2] // GW
    ng = ngq + kvw_ref.shape[2] // GW
    nq = ngq * SLOT
    nc = ng * SLOT
    nh = nc // 2
    row_chunks = rows // BLK

    section = lax.axis_index("section")
    me = lax.axis_index("rep")
    core = me % 2
    chip = me // 2
    pos = chip + (chip // hops) * (hops + chips - 1 - 2 * chip)
    partner = 2 * chip + (1 - core)

    def rep_at(place, which):
        return 2 * chip_at((place + chips) % chips, chips) + which

    towards = (rep_at(pos + 1, core), rep_at(pos - 1, core))

    barrier = pltpu.get_barrier_semaphore()
    for other in towards + (partner,):
        pl.semaphore_signal(barrier, 1, device_id={"rep": other}, device_id_type=MESH)

    @pl.when(section > 0)
    def _():
        pl.semaphore_signal(
            barrier, 1, device_id={"section": section - 1}, device_id_type=MESH
        )

    @pl.when(section < sections - 1)
    def _():
        pl.semaphore_signal(
            barrier, 1, device_id={"section": section + 1}, device_id_type=MESH
        )

    def own(g):
        if g < ngq:
            return qw_ref.at[0, :, pl.ds(g * GW, GW)]
        return kvw_ref.at[0, :, pl.ds((g - ngq) * GW, GW)]

    def depth_of(block):
        return pl.ds(pl.multiple_of(block * depth, depth), depth)

    def columns_of(c):
        return pl.ds(pl.multiple_of((c % SLOT) * CW, CW), CW)

    def slot(g, block):
        return w.at[g, depth_of(block), :]

    def piece(c, block):
        return w.at[c // SLOT, depth_of(block), columns_of(c)]

    def last_part(d, which, p):
        return last_w.at[d, depth_of(which), pl.ds(p * HALF, HALF)]

    keep = pltpu.make_async_copy(cache_ref, rebuilt_ref, keep_sem)
    gain_copy = pltpu.make_async_copy(gain_hbm, gain_ref, small_sem.at[0])
    small = [gain_copy]
    for g in range(ng):
        source, first = (qb_hbm, g) if g < ngq else (kvb_hbm, g - ngq)
        small.append(
            pltpu.make_async_copy(source.at[:, pl.ds(first * GW, GW)], bias.at[g], small_sem.at[1])
        )
    own_locals = [
        pltpu.make_async_copy(own(g), slot(g, me), local_sem.at[min(g, 1)]) for g in range(ng)
    ]

    sides = (section + sections - 1) // sections + (2 * sections - 2 - section) // sections
    own_locals[0].start()
    pl.semaphore_wait(barrier, 3 + sides)
    own_locals[0].wait()

    def list_copy(i):
        return pltpu.make_async_remote_copy(
            src_ref=lists_ref[i],
            dst_ref=lists[i],
            send_sem=list_send.at[i],
            recv_sem=list_recv.at[i],
            device_id={"section": section + 1},
            device_id_type=MESH,
        )

    def row_copy(j):
        return pltpu.make_async_remote_copy(
            src_ref=payload_ref.at[0, pl.ds(j * BLK, BLK), :],
            dst_ref=values.at[pl.ds(j * BLK, BLK), :],
            send_sem=row_send,
            recv_sem=row_recv.at[j],
            device_id={"section": section + 1},
            device_id_type=MESH,
        )

    for g in range(ng):
        source = own(g) if g else slot(g, me)
        for d in range(2):
            pltpu.make_async_remote_copy(
                src_ref=source,
                dst_ref=slot(g, me),
                send_sem=own_send,
                recv_sem=ring_recv.at[0, g],
                device_id={"rep": towards[d]},
                device_id_type=MESH,
            ).start()
        if g == 0:

            @pl.when(section < sections - 1)
            def _():
                for j in range(row_chunks):
                    row_copy(j).start()
                    if j == 0:
                        for i in range(len(lists)):
                            list_copy(i).start()

            keep.start()
            for copy in small:
                copy.start()

        pltpu.make_async_remote_copy(
            src_ref=source,
            dst_ref=slot(g, me),
            send_sem=own_send,
            recv_sem=pair_recv.at[g],
            device_id={"rep": partner},
            device_id_type=MESH,
        ).start()
        if g:
            own_locals[g].start()

    @pl.when(section == 0)
    def _():
        for ref in lists:
            ref[...] = jnp.zeros_like(ref)

        @pl.loop(0, rows // TILE)
        def _(i):
            values[pl.ds(i * TILE, TILE), :] = jnp.zeros((TILE, feature), values.dtype)

    def landed(sem, blocks, width=GW, slots=1):
        part = w.at[pl.ds(0, slots), pl.ds(0, blocks * depth), pl.ds(0, width)]
        pltpu.make_async_copy(part, part, sem).wait()

    gain_copy.wait()
    pltpu.make_async_copy(bias, bias, small_sem.at[1]).wait()
    keep.wait()
    landed(local_sem.at[1], 1, slots=ng - 1)

    def block_of(d, t, which):
        return rep_at(pos - t if d == 0 else pos + t, which)

    def pass_on(here, recv_sem, target):
        pltpu.make_async_remote_copy(
            src_ref=here,
            dst_ref=here,
            send_sem=pass_send,
            recv_sem=recv_sem,
            device_id={"rep": target},
            device_id_type=MESH,
        ).start()

    def rebuild(j):
        @pl.when(section > 0)
        def _():
            if j == 0:
                for i in range(len(lists)):
                    list_copy(i).wait_recv()
            row_copy(j).wait_recv()

        got_rows, got_ids, got_scales, got_counts, got_rcounts = lists
        count = got_counts[...]
        factor = jnp.zeros((1, 1), jnp.float32)
        for i in range(most_blk):
            live = jnp.logical_and(got_ids[:, i : i + 1] == j, count > i)
            scale = got_scales[:, i : i + 1].astype(jnp.float32) / 4096.0
            factor = factor + jnp.where(live, scale, 0.0)

        @pl.loop(0, BLK // TILE)
        def _(i):
            first = j * BLK + i * TILE
            here = pl.ds(pl.multiple_of(first, TILE), TILE)
            ids = got_rows[...]
            lanes = lax.broadcasted_iota(jnp.int32, ids.shape, 1)
            ids = jnp.where(lanes < got_rcounts[...], ids, -1)
            number = first + lax.broadcasted_iota(jnp.int32, (TILE, ids.shape[1]), 0)
            match = jnp.where(ids == number, 1.0, 0.0)
            hit = jnp.max(match, axis=1, keepdims=True) > 0.0
            got = values[here, :].astype(jnp.float32)
            delta = (got * factor).astype(jnp.bfloat16).astype(jnp.float32)
            mixed = jnp.where(hit, got, rebuilt_ref[0, here, :].astype(jnp.float32) + delta)
            rebuilt = mixed.astype(jnp.bfloat16)
            rebuilt_ref[0, here, :] = rebuilt
            wide = rebuilt.astype(jnp.float32)
            mean = jnp.sum(wide * wide, axis=1, keepdims=True) / feature
            scale_rows = lax.rsqrt(mean + EPSILON)
            result = (wide * scale_rows * gain_ref[...]).astype(jnp.bfloat16)
            for k in range(chips):
                normed[k, here, :] = result[:, 2 * depth * k : 2 * depth * (k + 1)]

    far = chip_at((pos + hops) % chips, chips)
    wide_depth = 2 * depth
    half = rows // 2

    def term(which, g, columns, first):
        rows_here = pl.ds(pl.multiple_of(which * wide_depth, wide_depth), wide_depth)
        return jnp.dot(
            normed[which, first : first + half, :],
            w[g, rows_here, columns],
            preferred_element_type=jnp.float32,
        )

    def near(g, columns, first):
        total = bias[g, :, columns]
        for step in range(1, chips):
            total = total + term((far + step) % chips, g, columns, first)
        return total

    def start(g):
        landed(pair_recv.at[g], 2 * hops - 1)
        early[g] = near(g, slice(None), 0)

    marks = [(j + 1) * ng // row_chunks for j in range(row_chunks)]
    marks[-1] = ng
    ready = marks[row_chunks // 2 - 1]
    per_step = -(-ng // (ng - ready))
    for t in range(1, hops):
        done = 0
        for j, mark in enumerate(marks):

            @pl.loop(done, mark)
            def _(g):
                landed(ring_recv.at[t - 1, g], 2)
                for d in range(2):
                    here = slot(g, block_of(d, t, core))
                    if t + 1 < hops:
                        pass_on(here, ring_recv.at[t, g], towards[d])
                    else:
                        for k in range(SLOT):
                            c = g * SLOT + k
                            last = nh - 1 + d * nh

                            @pl.when((c < last) if d == 0 else ((c >= nh) & (c < last)))
                            def _():
                                pass_on(
                                    piece(c, block_of(d, t, core)),
                                    far_recv.at[c - d * nh],
                                    towards[d],
                                )

                            if k == last % SLOT:

                                @pl.when(c == last)
                                def _():
                                    for p in range(CW // HALF):
                                        pltpu.make_async_remote_copy(
                                            src_ref=w.at[
                                                last // SLOT,
                                                depth_of(block_of(d, t, core)),
                                                pl.ds(k * CW + p * HALF, HALF),
                                            ],
                                            dst_ref=last_part(d, core, p),
                                            send_sem=pass_send,
                                            recv_sem=far_recv.at[nh - 1 + p],
                                            device_id={"rep": towards[d]},
                                            device_id_type=MESH,
                                        ).start()

                    pass_on(here, pair_recv.at[g], partner)
                if t + 1 == hops and (t > 1 or done >= ready):
                    for k in range(per_step):
                        other = (g - ready) * per_step + k

                        @pl.when(jnp.logical_and(other >= 0, other < ng))
                        def _():
                            start(other)

            done = mark
            if t == 1:
                rebuild(j)

    def partial(i):
        for d in range(2):
            c = i + d * nh
            sums[i % 2, d] = near(c // SLOT, columns_of(c), half)

    def finish(i):
        for d in range(2):
            c = i + d * nh
            for first in (0, half):
                if first == 0:
                    total = early[c // SLOT, :, columns_of(c)]
                else:
                    total = sums[i % 2, d]
                total = total + term(far, c // SLOT, columns_of(c), first)
                result = total.astype(jnp.bfloat16)
                here = slice(first, first + half)

                @pl.when(c < nq)
                def _():
                    q_ref[0, here, pl.ds(pl.multiple_of(c * CW, CW), CW)] = result

                @pl.when(c >= nq)
                def _():
                    kv_ref[0, here, pl.ds(pl.multiple_of((c - nq) * CW, CW), CW)] = result

    def arrived(i):
        landed(far_recv.at[i], 2, CW)
        for d in range(2):
            pass_on(piece(i + d * nh, block_of(d, hops, core)), far_pair_recv.at[i], partner)

    partial(0)
    last_normed[...] = normed[far]
    for d in range(2):
        c = nh - 1 + d * nh
        columns = slice((c % SLOT) * CW, (c % SLOT + 1) * CW)
        last_sums[d, :half, :] = early[c // SLOT, :, columns]
        last_sums[d, half:, :] = near(c // SLOT, columns, half)

    @pl.loop(0, nh - 1)
    def _(i):
        arrived(i)

        @pl.when(i + 1 < nh - 1)
        def _():
            partial(i + 1)

        landed(far_pair_recv.at[i], 2, CW)
        finish(i)

    for p in range(CW // HALF):
        landed(far_recv.at[nh - 1 + p], 2, HALF)
        for d in range(2):
            pass_on(last_part(d, core, p), far_pair_recv.at[nh - 1 + p], partner)

    landed(own_send, 3, slots=ng)

    @pl.when(section < sections - 1)
    def _():
        for i in range(len(lists)):
            list_copy(i).wait_send()
        pltpu.make_async_copy(values, values, row_send).wait()

    landed(pass_send, 4 * hops - 4, slots=ng)
    for p in range(CW // HALF):
        landed(far_pair_recv.at[nh - 1 + p], 2, HALF)


def put_out(
    parts,
    rebuilt_ref,
    q_ref,
    kv_ref,
    last_w,
    last_normed,
    last_sums,
    rebuilt_out,
    q_out,
    kv_out,
    last,
    sem,
):
    rows = q_ref.shape[1]
    nq = q_ref.shape[2] // CW
    nc = nq + kv_ref.shape[2] // CW
    last_pieces = (nc // 2 - 1, nc - 1)

    step = rows // parts

    def out(source, target, base, k):
        count = source.shape[2] // CW
        cuts = [c - base for c in last_pieces if base <= c < base + count]
        for first, stop in zip([0] + [c + 1 for c in cuts], cuts + [count]):
            if first < stop:
                columns = pl.ds(first * CW, (stop - first) * CW)
                for j in range(parts):
                    here = pl.ds(j * step, step)
                    pltpu.make_async_copy(
                        source.at[:, here, columns], target.at[:, here, columns], sem.at[k]
                    ).start()
        whole = source.at[:, :, pl.ds(0, (count - len(cuts)) * CW)]
        return pltpu.make_async_copy(whole, whole, sem.at[k])

    arrays = ((rebuilt_ref, rebuilt_out, nc), (q_ref, q_out, 0), (kv_ref, kv_out, nq))
    waits = [out(source, target, base, k) for k, (source, target, base) in enumerate(arrays)]
    for d, c in enumerate(last_pieces):
        total = last_sums[d] + jnp.dot(
            last_normed[...], last_w[d], preferred_element_type=jnp.float32
        )
        last[d] = total.astype(jnp.bfloat16)
        target, base = (q_out, 0) if c < nq else (kv_out, nq)
        pltpu.make_async_copy(
            last.at[d], target.at[0, :, pl.ds((c - base) * CW, CW)], sem.at[len(arrays)]
        ).start()
    for copy in waits:
        copy.wait()
    pltpu.make_async_copy(last, last, sem.at[len(arrays)]).wait()


def body(
    cache,
    payload,
    block_ids,
    block_counts,
    block_scales,
    refresh_ids,
    refresh_counts,
    norm_gain,
    query_weight,
    query_bias,
    kv_weight,
    kv_bias,
):
    sections = lax.axis_size("section")
    reps = lax.axis_size("rep")
    rows, feature = cache.shape[1:]
    depth = query_weight.shape[1]
    queries = query_weight.shape[2]
    keys = kv_weight.shape[2]
    most_blk = block_ids.shape[2]
    ng = (queries + keys) // GW
    nh = ng * SLOT // 2
    hops = reps // 4
    row_chunks = rows // BLK

    lists = (refresh_ids[0], block_ids[0], block_scales[0], block_counts, refresh_counts)
    vmem = pl.BlockSpec(memory_space=pltpu.VMEM)
    anywhere = pl.BlockSpec(memory_space=pltpu.HBM)
    dma = pltpu.SemaphoreType.DMA
    results = pl.pallas_call(
        functools.partial(kernel, sections, reps, most_blk),
        out_shape=(
            pltpu.VMEM(cache.shape, cache.dtype),
            pltpu.VMEM((1, rows, queries), cache.dtype),
            pltpu.VMEM((1, rows, keys), cache.dtype),
            pltpu.VMEM((2, 2 * depth, CW), jnp.bfloat16),
            pltpu.VMEM((rows, 2 * depth), jnp.bfloat16),
            pltpu.VMEM((2, rows, CW), jnp.float32),
        ),
        in_specs=[(anywhere,) * len(lists)] + [anywhere] * 7,
        out_specs=(vmem,) * 6,
        scratch_shapes=[
            pltpu.VMEM((ng, reps * depth, GW), jnp.bfloat16),
            pltpu.VMEM((reps // 2, rows, 2 * depth), jnp.bfloat16),
            pltpu.VMEM((ng, rows // 2, GW), jnp.float32),
            pltpu.VMEM((2, 2, rows // 2, CW), jnp.float32),
            pltpu.VMEM((rows, feature), jnp.bfloat16),
            pltpu.VMEM(norm_gain.shape, jnp.float32),
            pltpu.VMEM((ng, 1, GW), jnp.float32),
            tuple(pltpu.VMEM(x.shape, x.dtype) for x in lists),
            dma((2,)),
            dma,
            dma((2,)),
            dma,
            dma((row_chunks,)),
            dma((len(lists),)),
            dma((len(lists),)),
            dma,
            dma,
            dma((hops - 1, ng)),
            dma((ng,)),
            dma((nh - 1 + CW // HALF,)),
            dma((nh - 1 + CW // HALF,)),
        ],
        compiler_params=pltpu.CompilerParams(
            collective_id=0, has_side_effects=True, vmem_limit_bytes=KERNEL_VMEM
        ),
    )(lists, payload, cache, norm_gain, query_weight, query_bias, kv_weight, kv_bias)
    return tuple(
        pl.pallas_call(
            functools.partial(put_out, 2),
            out_shape=tuple(pltpu.HBM(x.shape, x.dtype) for x in results[:3]),
            in_specs=[vmem] * len(results),
            out_specs=(anywhere,) * 3,
            scratch_shapes=[
                pltpu.VMEM((2, rows, CW), jnp.bfloat16),
                dma((4,)),
            ],
            compiler_params=pltpu.CompilerParams(vmem_limit_bytes=OUT_VMEM),
        )(*results)
    )


def solution(mesh):
    in_specs = (
        P("section", "rep", None),
        P("section", "rep", None),
        P("section", "rep", None),
        P("section", "rep"),
        P("section", "rep", None),
        P("section", "rep", None),
        P("section", "rep"),
        P("section", None),
        P("section", "rep", None),
        P("section", None),
        P("section", "rep", None),
        P("section", None),
    )
    out_specs = (P("section", "rep", None), P("section", "rep", None), P("section", "rep", None))
    return jax.shard_map(body, mesh=mesh, in_specs=in_specs, out_specs=out_specs, check_vma=False)
```

```python
import functools

import jax
import jax.numpy as jnp
from jax import lax
from jax.experimental import pallas as pl
from jax.experimental.pallas import tpu as pltpu
from jax.sharding import PartitionSpec as P

BLK = 128
HALF = 128
CW = 256
PARTS = 2 * CW // HALF
SLOT = 2
GW = SLOT * CW
TILE = 16
EPSILON = 1e-06
KERNEL_VMEM = 100 * 512 * 1024
OUT_VMEM = 3 * 1024 * 1024
MESH = pl.DeviceIdType.MESH


def chip_at(pos, chips):
    half = chips // 2
    back = pos // half
    return pos + back * (half + chips - 1 - 2 * pos)


def kernel(
    sections,
    reps,
    most_blk,
    lists_ref,
    payload_ref,
    cache_ref,
    gain_hbm,
    qw_ref,
    qb_hbm,
    kvw_ref,
    kvb_hbm,
    rebuilt_ref,
    q_ref,
    kv_ref,
    last_w,
    last_normed,
    last_sums,
    w,
    normed,
    early,
    sums,
    values,
    gain_ref,
    bias,
    lists,
    local_sem,
    keep_sem,
    small_sem,
    row_send,
    row_recv,
    list_send,
    list_recv,
    own_send,
    pass_send,
    ring_recv,
    pair_recv,
    far_recv,
    far_pair_recv,
):
    chips = reps // 2
    hops = chips // 2
    depth = qw_ref.shape[1]
    rows = payload_ref.shape[1]
    feature = payload_ref.shape[2]
    ngq = qw_ref.shape[2] // GW
    ng = ngq + kvw_ref.shape[2] // GW
    nq = ngq * SLOT
    nc = ng * SLOT
    nh = nc // 2
    row_chunks = rows // BLK

    section = lax.axis_index("section")
    me = lax.axis_index("rep")
    core = me % 2
    chip = me // 2
    pos = chip + (chip // hops) * (hops + chips - 1 - 2 * chip)
    partner = 2 * chip + (1 - core)

    def rep_at(place, which):
        return 2 * chip_at((place + chips) % chips, chips) + which

    towards = (rep_at(pos + 1, core), rep_at(pos - 1, core))

    barrier = pltpu.get_barrier_semaphore()
    for other in towards + (partner,):
        pl.semaphore_signal(barrier, 1, device_id={"rep": other}, device_id_type=MESH)

    @pl.when(section > 0)
    def _():
        pl.semaphore_signal(
            barrier, 1, device_id={"section": section - 1}, device_id_type=MESH
        )

    @pl.when(section < sections - 1)
    def _():
        pl.semaphore_signal(
            barrier, 1, device_id={"section": section + 1}, device_id_type=MESH
        )

    def own(g):
        if g < ngq:
            return qw_ref.at[0, :, pl.ds(g * GW, GW)]
        return kvw_ref.at[0, :, pl.ds((g - ngq) * GW, GW)]

    def depth_of(block):
        return pl.ds(pl.multiple_of(block * depth, depth), depth)

    def columns_of(c):
        return pl.ds(pl.multiple_of((c % SLOT) * CW, CW), CW)

    def slot(g, block):
        return w.at[g, depth_of(block), :]

    def piece(c, block):
        return w.at[c // SLOT, depth_of(block), columns_of(c)]

    def half_of(block, p):
        first = block * depth + p % 2 * (depth // 2)
        return pl.ds(pl.multiple_of(first, depth // 2), depth // 2)

    def last_part(d, which, p):
        return last_w.at[d, half_of(which, p), pl.ds(p // 2 * HALF, HALF)]

    keep = pltpu.make_async_copy(cache_ref, rebuilt_ref, keep_sem)
    gain_copy = pltpu.make_async_copy(gain_hbm, gain_ref, small_sem.at[0])
    small = [gain_copy]
    for g in range(ng):
        source, first = (qb_hbm, g) if g < ngq else (kvb_hbm, g - ngq)
        small.append(
            pltpu.make_async_copy(source.at[:, pl.ds(first * GW, GW)], bias.at[g], small_sem.at[1])
        )
    own_locals = [
        pltpu.make_async_copy(own(g), slot(g, me), local_sem.at[min(g, 1)]) for g in range(ng)
    ]

    sides = (section + sections - 1) // sections + (2 * sections - 2 - section) // sections
    own_locals[0].start()
    pl.semaphore_wait(barrier, 3 + sides)
    own_locals[0].wait()

    def list_copy(i):
        return pltpu.make_async_remote_copy(
            src_ref=lists_ref[i],
            dst_ref=lists[i],
            send_sem=list_send.at[i],
            recv_sem=list_recv.at[i],
            device_id={"section": section + 1},
            device_id_type=MESH,
        )

    def row_copy(j):
        return pltpu.make_async_remote_copy(
            src_ref=payload_ref.at[0, pl.ds(j * BLK, BLK), :],
            dst_ref=values.at[pl.ds(j * BLK, BLK), :],
            send_sem=row_send,
            recv_sem=row_recv.at[j],
            device_id={"section": section + 1},
            device_id_type=MESH,
        )

    for g in range(ng):
        source = own(g) if g else slot(g, me)
        for d in range(2):
            pltpu.make_async_remote_copy(
                src_ref=source,
                dst_ref=slot(g, me),
                send_sem=own_send,
                recv_sem=ring_recv.at[0, g],
                device_id={"rep": towards[d]},
                device_id_type=MESH,
            ).start()
        if g == 0:

            @pl.when(section < sections - 1)
            def _():
                for j in range(row_chunks):
                    row_copy(j).start()
                    if j == 0:
                        for i in range(len(lists)):
                            list_copy(i).start()

            keep.start()
            for copy in small:
                copy.start()

        pltpu.make_async_remote_copy(
            src_ref=source,
            dst_ref=slot(g, me),
            send_sem=own_send,
            recv_sem=pair_recv.at[g],
            device_id={"rep": partner},
            device_id_type=MESH,
        ).start()
        if g:
            own_locals[g].start()

    @pl.when(section == 0)
    def _():
        for ref in lists:
            ref[...] = jnp.zeros_like(ref)

        @pl.loop(0, rows // TILE)
        def _(i):
            values[pl.ds(i * TILE, TILE), :] = jnp.zeros((TILE, feature), values.dtype)

    def landed(sem, blocks, width=GW, slots=1):
        part = w.at[pl.ds(0, slots), pl.ds(0, blocks * depth), pl.ds(0, width)]
        pltpu.make_async_copy(part, part, sem).wait()

    gain_copy.wait()
    pltpu.make_async_copy(bias, bias, small_sem.at[1]).wait()
    keep.wait()
    landed(local_sem.at[1], 1, slots=ng - 1)

    def block_of(d, t, which):
        return rep_at(pos - t if d == 0 else pos + t, which)

    def pass_on(here, recv_sem, target):
        pltpu.make_async_remote_copy(
            src_ref=here,
            dst_ref=here,
            send_sem=pass_send,
            recv_sem=recv_sem,
            device_id={"rep": target},
            device_id_type=MESH,
        ).start()

    def rebuild(j):
        @pl.when(section > 0)
        def _():
            if j == 0:
                for i in range(len(lists)):
                    list_copy(i).wait_recv()
            row_copy(j).wait_recv()

        got_rows, got_ids, got_scales, got_counts, got_rcounts = lists
        count = got_counts[...]
        factor = jnp.zeros((1, 1), jnp.float32)
        for i in range(most_blk):
            live = jnp.logical_and(got_ids[:, i : i + 1] == j, count > i)
            scale = got_scales[:, i : i + 1].astype(jnp.float32) / 4096.0
            factor = factor + jnp.where(live, scale, 0.0)

        @pl.loop(0, BLK // TILE)
        def _(i):
            first = j * BLK + i * TILE
            here = pl.ds(pl.multiple_of(first, TILE), TILE)
            ids = got_rows[...]
            lanes = lax.broadcasted_iota(jnp.int32, ids.shape, 1)
            ids = jnp.where(lanes < got_rcounts[...], ids, -1)
            number = first + lax.broadcasted_iota(jnp.int32, (TILE, ids.shape[1]), 0)
            match = jnp.where(ids == number, 1.0, 0.0)
            hit = jnp.max(match, axis=1, keepdims=True) > 0.0
            got = values[here, :].astype(jnp.float32)
            delta = (got * factor).astype(jnp.bfloat16).astype(jnp.float32)
            mixed = jnp.where(hit, got, rebuilt_ref[0, here, :].astype(jnp.float32) + delta)
            rebuilt = mixed.astype(jnp.bfloat16)
            rebuilt_ref[0, here, :] = rebuilt
            wide = rebuilt.astype(jnp.float32)
            mean = jnp.sum(wide * wide, axis=1, keepdims=True) / feature
            scale_rows = lax.rsqrt(mean + EPSILON)
            result = (wide * scale_rows * gain_ref[...]).astype(jnp.bfloat16)
            for k in range(chips):
                normed[k, here, :] = result[:, 2 * depth * k : 2 * depth * (k + 1)]

    far = chip_at((pos + hops) % chips, chips)
    wide_depth = 2 * depth
    half = rows // 2

    def term(which, g, columns, first):
        rows_here = pl.ds(pl.multiple_of(which * wide_depth, wide_depth), wide_depth)
        return jnp.dot(
            normed[which, first : first + half, :],
            w[g, rows_here, columns],
            preferred_element_type=jnp.float32,
        )

    def near(g, columns, first):
        total = bias[g, :, columns]
        for step in range(1, chips):
            total = total + term((far + step) % chips, g, columns, first)
        return total

    def start(g):
        landed(pair_recv.at[g], 2 * hops - 1)
        early[g] = near(g, slice(None), 0)

    marks = [(j + 1) * ng // row_chunks for j in range(row_chunks)]
    marks[-1] = ng
    ready = marks[row_chunks // 2 - 1]
    per_step = -(-ng // (ng - ready))
    for t in range(1, hops):
        done = 0
        for j, mark in enumerate(marks):

            @pl.loop(done, mark)
            def _(g):
                landed(ring_recv.at[t - 1, g], 2)
                for d in range(2):
                    here = slot(g, block_of(d, t, core))
                    if t + 1 < hops:
                        pass_on(here, ring_recv.at[t, g], towards[d])
                    else:
                        for k in range(SLOT):
                            c = g * SLOT + k
                            last = nh - 1 + d * nh

                            @pl.when((c < last) if d == 0 else ((c >= nh) & (c < last)))
                            def _():
                                pass_on(
                                    piece(c, block_of(d, t, core)),
                                    far_recv.at[c - d * nh],
                                    towards[d],
                                )

                            if k == last % SLOT:

                                @pl.when(c == last)
                                def _():
                                    for p in range(PARTS):
                                        pltpu.make_async_remote_copy(
                                            src_ref=w.at[
                                                last // SLOT,
                                                half_of(block_of(d, t, core), p),
                                                pl.ds(k * CW + p // 2 * HALF, HALF),
                                            ],
                                            dst_ref=last_part(d, core, p),
                                            send_sem=pass_send,
                                            recv_sem=far_recv.at[nh - 1 + p],
                                            device_id={"rep": towards[d]},
                                            device_id_type=MESH,
                                        ).start()

                    pass_on(here, pair_recv.at[g], partner)
                if t + 1 == hops and (t > 1 or done >= ready):
                    for k in range(per_step):
                        other = (g - ready) * per_step + k

                        @pl.when(jnp.logical_and(other >= 0, other < ng))
                        def _():
                            start(other)

            done = mark
            if t == 1:
                rebuild(j)

    def partial(i):
        for d in range(2):
            c = i + d * nh
            sums[i % 2, d] = near(c // SLOT, columns_of(c), half)

    def finish(i):
        for d in range(2):
            c = i + d * nh
            for first in (0, half):
                if first == 0:
                    total = early[c // SLOT, :, columns_of(c)]
                else:
                    total = sums[i % 2, d]
                total = total + term(far, c // SLOT, columns_of(c), first)
                result = total.astype(jnp.bfloat16)
                here = slice(first, first + half)

                @pl.when(c < nq)
                def _():
                    q_ref[0, here, pl.ds(pl.multiple_of(c * CW, CW), CW)] = result

                @pl.when(c >= nq)
                def _():
                    kv_ref[0, here, pl.ds(pl.multiple_of((c - nq) * CW, CW), CW)] = result

    def arrived(i):
        landed(far_recv.at[i], 2, CW)
        for d in range(2):
            pass_on(piece(i + d * nh, block_of(d, hops, core)), far_pair_recv.at[i], partner)

    partial(0)
    last_normed[...] = normed[far]
    for d in range(2):
        c = nh - 1 + d * nh
        columns = slice((c % SLOT) * CW, (c % SLOT + 1) * CW)
        last_sums[d, :half, :] = early[c // SLOT, :, columns]
        last_sums[d, half:, :] = near(c // SLOT, columns, half)

    @pl.loop(0, nh - 1)
    def _(i):
        arrived(i)

        @pl.when(i + 1 < nh - 1)
        def _():
            partial(i + 1)

        landed(far_pair_recv.at[i], 2, CW)
        finish(i)

    for p in range(PARTS):
        landed(far_recv.at[nh - 1 + p], 1, HALF)
        for d in range(2):
            pass_on(last_part(d, core, p), far_pair_recv.at[nh - 1 + p], partner)

    landed(own_send, 3, slots=ng)

    @pl.when(section < sections - 1)
    def _():
        for i in range(len(lists)):
            list_copy(i).wait_send()
        pltpu.make_async_copy(values, values, row_send).wait()

    landed(pass_send, 4 * hops - 4, slots=ng)
    for p in range(PARTS):
        landed(far_pair_recv.at[nh - 1 + p], 1, HALF)


def put_out(
    parts,
    rebuilt_ref,
    q_ref,
    kv_ref,
    last_w,
    last_normed,
    last_sums,
    rebuilt_out,
    q_out,
    kv_out,
    last,
    sem,
):
    rows = q_ref.shape[1]
    nq = q_ref.shape[2] // CW
    nc = nq + kv_ref.shape[2] // CW
    last_pieces = (nc // 2 - 1, nc - 1)

    step = rows // parts

    def out(source, target, base, k):
        count = source.shape[2] // CW
        cuts = [c - base for c in last_pieces if base <= c < base + count]
        for first, stop in zip([0] + [c + 1 for c in cuts], cuts + [count]):
            if first < stop:
                columns = pl.ds(first * CW, (stop - first) * CW)
                for j in range(parts):
                    here = pl.ds(j * step, step)
                    pltpu.make_async_copy(
                        source.at[:, here, columns], target.at[:, here, columns], sem.at[k]
                    ).start()
        whole = source.at[:, :, pl.ds(0, (count - len(cuts)) * CW)]
        return pltpu.make_async_copy(whole, whole, sem.at[k])

    arrays = ((rebuilt_ref, rebuilt_out, nc), (q_ref, q_out, 0), (kv_ref, kv_out, nq))
    waits = [out(source, target, base, k) for k, (source, target, base) in enumerate(arrays)]
    for d, c in enumerate(last_pieces):
        total = last_sums[d] + jnp.dot(
            last_normed[...], last_w[d], preferred_element_type=jnp.float32
        )
        last[d] = total.astype(jnp.bfloat16)
        target, base = (q_out, 0) if c < nq else (kv_out, nq)
        pltpu.make_async_copy(
            last.at[d], target.at[0, :, pl.ds((c - base) * CW, CW)], sem.at[len(arrays)]
        ).start()
    for copy in waits:
        copy.wait()
    pltpu.make_async_copy(last, last, sem.at[len(arrays)]).wait()


def body(
    cache,
    payload,
    block_ids,
    block_counts,
    block_scales,
    refresh_ids,
    refresh_counts,
    norm_gain,
    query_weight,
    query_bias,
    kv_weight,
    kv_bias,
):
    sections = lax.axis_size("section")
    reps = lax.axis_size("rep")
    rows, feature = cache.shape[1:]
    depth = query_weight.shape[1]
    queries = query_weight.shape[2]
    keys = kv_weight.shape[2]
    most_blk = block_ids.shape[2]
    ng = (queries + keys) // GW
    nh = ng * SLOT // 2
    hops = reps // 4
    row_chunks = rows // BLK

    lists = (refresh_ids[0], block_ids[0], block_scales[0], block_counts, refresh_counts)
    vmem = pl.BlockSpec(memory_space=pltpu.VMEM)
    anywhere = pl.BlockSpec(memory_space=pltpu.HBM)
    dma = pltpu.SemaphoreType.DMA
    results = pl.pallas_call(
        functools.partial(kernel, sections, reps, most_blk),
        out_shape=(
            pltpu.VMEM(cache.shape, cache.dtype),
            pltpu.VMEM((1, rows, queries), cache.dtype),
            pltpu.VMEM((1, rows, keys), cache.dtype),
            pltpu.VMEM((2, 2 * depth, CW), jnp.bfloat16),
            pltpu.VMEM((rows, 2 * depth), jnp.bfloat16),
            pltpu.VMEM((2, rows, CW), jnp.float32),
        ),
        in_specs=[(anywhere,) * len(lists)] + [anywhere] * 7,
        out_specs=(vmem,) * 6,
        scratch_shapes=[
            pltpu.VMEM((ng, reps * depth, GW), jnp.bfloat16),
            pltpu.VMEM((reps // 2, rows, 2 * depth), jnp.bfloat16),
            pltpu.VMEM((ng, rows // 2, GW), jnp.float32),
            pltpu.VMEM((2, 2, rows // 2, CW), jnp.float32),
            pltpu.VMEM((rows, feature), jnp.bfloat16),
            pltpu.VMEM(norm_gain.shape, jnp.float32),
            pltpu.VMEM((ng, 1, GW), jnp.float32),
            tuple(pltpu.VMEM(x.shape, x.dtype) for x in lists),
            dma((2,)),
            dma,
            dma((2,)),
            dma,
            dma((row_chunks,)),
            dma((len(lists),)),
            dma((len(lists),)),
            dma,
            dma,
            dma((hops - 1, ng)),
            dma((ng,)),
            dma((nh - 1 + PARTS,)),
            dma((nh - 1 + PARTS,)),
        ],
        compiler_params=pltpu.CompilerParams(
            collective_id=0, has_side_effects=True, vmem_limit_bytes=KERNEL_VMEM
        ),
    )(lists, payload, cache, norm_gain, query_weight, query_bias, kv_weight, kv_bias)
    return tuple(
        pl.pallas_call(
            functools.partial(put_out, 2),
            out_shape=tuple(pltpu.HBM(x.shape, x.dtype) for x in results[:3]),
            in_specs=[vmem] * len(results),
            out_specs=(anywhere,) * 3,
            scratch_shapes=[
                pltpu.VMEM((2, rows, CW), jnp.bfloat16),
                dma((4,)),
            ],
            compiler_params=pltpu.CompilerParams(vmem_limit_bytes=OUT_VMEM),
        )(*results)
    )


def solution(mesh):
    in_specs = (
        P("section", "rep", None),
        P("section", "rep", None),
        P("section", "rep", None),
        P("section", "rep"),
        P("section", "rep", None),
        P("section", "rep", None),
        P("section", "rep"),
        P("section", None),
        P("section", "rep", None),
        P("section", None),
        P("section", "rep", None),
        P("section", None),
    )
    out_specs = (P("section", "rep", None), P("section", "rep", None), P("section", "rep", None))
    return jax.shard_map(body, mesh=mesh, in_specs=in_specs, out_specs=out_specs, check_vma=False)
```

```python
import functools

import jax
import jax.numpy as jnp
from jax import lax
from jax.experimental import pallas as pl
from jax.experimental.pallas import tpu as pltpu
from jax.sharding import PartitionSpec as P

BLK = 128
HALF = 128
CW = 256
PARTS = 2 * CW // HALF
SLOT = 2
GW = SLOT * CW
TILE = 16
EPSILON = 1e-06
KERNEL_VMEM = 100 * 512 * 1024
OUT_VMEM = 3 * 1024 * 1024
MESH = pl.DeviceIdType.MESH


def chip_at(pos, chips):
    half = chips // 2
    back = pos // half
    return pos + back * (half + chips - 1 - 2 * pos)


def kernel(
    sections,
    reps,
    most_blk,
    lists_ref,
    payload_ref,
    cache_ref,
    gain_hbm,
    qw_ref,
    qb_hbm,
    kvw_ref,
    kvb_hbm,
    rebuilt_ref,
    q_ref,
    kv_ref,
    last_w,
    last_normed,
    last_sums,
    w,
    normed,
    early,
    sums,
    values,
    gain_ref,
    bias,
    lists,
    local_sem,
    keep_sem,
    small_sem,
    row_send,
    row_recv,
    list_send,
    list_recv,
    own_send,
    pass_send,
    ring_recv,
    pair_recv,
    far_recv,
):
    chips = reps // 2
    hops = chips // 2
    depth = qw_ref.shape[1]
    rows = payload_ref.shape[1]
    feature = payload_ref.shape[2]
    ngq = qw_ref.shape[2] // GW
    ng = ngq + kvw_ref.shape[2] // GW
    nq = ngq * SLOT
    nc = ng * SLOT
    nh = nc // 2
    row_chunks = rows // BLK

    section = lax.axis_index("section")
    me = lax.axis_index("rep")
    core = me % 2
    chip = me // 2
    pos = chip + (chip // hops) * (hops + chips - 1 - 2 * chip)
    partner = 2 * chip + (1 - core)

    def rep_at(place, which):
        return 2 * chip_at((place + chips) % chips, chips) + which

    towards = (rep_at(pos + 1, core), rep_at(pos - 1, core))

    barrier = pltpu.get_barrier_semaphore()
    for other in towards + (partner,):
        pl.semaphore_signal(barrier, 1, device_id={"rep": other}, device_id_type=MESH)

    @pl.when(section > 0)
    def _():
        pl.semaphore_signal(
            barrier, 1, device_id={"section": section - 1}, device_id_type=MESH
        )

    @pl.when(section < sections - 1)
    def _():
        pl.semaphore_signal(
            barrier, 1, device_id={"section": section + 1}, device_id_type=MESH
        )

    def own(g):
        if g < ngq:
            return qw_ref.at[0, :, pl.ds(g * GW, GW)]
        return kvw_ref.at[0, :, pl.ds((g - ngq) * GW, GW)]

    def depth_of(block):
        return pl.ds(pl.multiple_of(block * depth, depth), depth)

    def columns_of(c):
        return pl.ds(pl.multiple_of((c % SLOT) * CW, CW), CW)

    def slot(g, block):
        return w.at[g, depth_of(block), :]

    def piece(c, block):
        return w.at[c // SLOT, depth_of(block), columns_of(c)]

    def half_of(block, p):
        first = block * depth + p % 2 * (depth // 2)
        return pl.ds(pl.multiple_of(first, depth // 2), depth // 2)

    def last_part(d, which, p):
        return last_w.at[d, half_of(which, p), pl.ds(p // 2 * HALF, HALF)]

    keep = pltpu.make_async_copy(cache_ref, rebuilt_ref, keep_sem)
    gain_copy = pltpu.make_async_copy(gain_hbm, gain_ref, small_sem.at[0])
    small = [gain_copy]
    for g in range(ng):
        source, first = (qb_hbm, g) if g < ngq else (kvb_hbm, g - ngq)
        small.append(
            pltpu.make_async_copy(source.at[:, pl.ds(first * GW, GW)], bias.at[g], small_sem.at[1])
        )
    own_locals = [
        pltpu.make_async_copy(own(g), slot(g, me), local_sem.at[min(g, 1)]) for g in range(ng)
    ]

    sides = (section + sections - 1) // sections + (2 * sections - 2 - section) // sections
    own_locals[0].start()
    pl.semaphore_wait(barrier, 3 + sides)
    own_locals[0].wait()

    def list_copy(i):
        return pltpu.make_async_remote_copy(
            src_ref=lists_ref[i],
            dst_ref=lists[i],
            send_sem=list_send.at[i],
            recv_sem=list_recv.at[i],
            device_id={"section": section + 1},
            device_id_type=MESH,
        )

    def row_copy(j):
        return pltpu.make_async_remote_copy(
            src_ref=payload_ref.at[0, pl.ds(j * BLK, BLK), :],
            dst_ref=values.at[pl.ds(j * BLK, BLK), :],
            send_sem=row_send,
            recv_sem=row_recv.at[j],
            device_id={"section": section + 1},
            device_id_type=MESH,
        )

    for g in range(ng):
        source = own(g) if g else slot(g, me)
        for d in range(2):
            pltpu.make_async_remote_copy(
                src_ref=source,
                dst_ref=slot(g, me),
                send_sem=own_send,
                recv_sem=ring_recv.at[0, g],
                device_id={"rep": towards[d]},
                device_id_type=MESH,
            ).start()
        if g == 0:

            @pl.when(section < sections - 1)
            def _():
                for j in range(row_chunks):
                    row_copy(j).start()
                    if j == 0:
                        for i in range(len(lists)):
                            list_copy(i).start()

            keep.start()
            for copy in small:
                copy.start()

        pltpu.make_async_remote_copy(
            src_ref=source,
            dst_ref=slot(g, me),
            send_sem=own_send,
            recv_sem=pair_recv.at[g],
            device_id={"rep": partner},
            device_id_type=MESH,
        ).start()
        if g:
            own_locals[g].start()

    @pl.when(section == 0)
    def _():
        for ref in lists:
            ref[...] = jnp.zeros_like(ref)

        @pl.loop(0, rows // TILE)
        def _(i):
            values[pl.ds(i * TILE, TILE), :] = jnp.zeros((TILE, feature), values.dtype)

    def landed(sem, blocks, width=GW, slots=1):
        part = w.at[pl.ds(0, slots), pl.ds(0, blocks * depth), pl.ds(0, width)]
        pltpu.make_async_copy(part, part, sem).wait()

    gain_copy.wait()
    pltpu.make_async_copy(bias, bias, small_sem.at[1]).wait()
    keep.wait()
    landed(local_sem.at[1], 1, slots=ng - 1)

    def block_of(d, t, which):
        return rep_at(pos - t if d == 0 else pos + t, which)

    def pass_on(here, recv_sem, target):
        pltpu.make_async_remote_copy(
            src_ref=here,
            dst_ref=here,
            send_sem=pass_send,
            recv_sem=recv_sem,
            device_id={"rep": target},
            device_id_type=MESH,
        ).start()

    def rebuild(j):
        @pl.when(section > 0)
        def _():
            if j == 0:
                for i in range(len(lists)):
                    list_copy(i).wait_recv()
            row_copy(j).wait_recv()

        got_rows, got_ids, got_scales, got_counts, got_rcounts = lists
        count = got_counts[...]
        factor = jnp.zeros((1, 1), jnp.float32)
        for i in range(most_blk):
            live = jnp.logical_and(got_ids[:, i : i + 1] == j, count > i)
            scale = got_scales[:, i : i + 1].astype(jnp.float32) / 4096.0
            factor = factor + jnp.where(live, scale, 0.0)

        @pl.loop(0, BLK // TILE)
        def _(i):
            first = j * BLK + i * TILE
            here = pl.ds(pl.multiple_of(first, TILE), TILE)
            ids = got_rows[...]
            lanes = lax.broadcasted_iota(jnp.int32, ids.shape, 1)
            ids = jnp.where(lanes < got_rcounts[...], ids, -1)
            number = first + lax.broadcasted_iota(jnp.int32, (TILE, ids.shape[1]), 0)
            match = jnp.where(ids == number, 1.0, 0.0)
            hit = jnp.max(match, axis=1, keepdims=True) > 0.0
            got = values[here, :].astype(jnp.float32)
            delta = (got * factor).astype(jnp.bfloat16).astype(jnp.float32)
            mixed = jnp.where(hit, got, rebuilt_ref[0, here, :].astype(jnp.float32) + delta)
            rebuilt = mixed.astype(jnp.bfloat16)
            rebuilt_ref[0, here, :] = rebuilt
            wide = rebuilt.astype(jnp.float32)
            mean = jnp.sum(wide * wide, axis=1, keepdims=True) / feature
            scale_rows = lax.rsqrt(mean + EPSILON)
            result = (wide * scale_rows * gain_ref[...]).astype(jnp.bfloat16)
            for k in range(chips):
                normed[k, here, :] = result[:, 2 * depth * k : 2 * depth * (k + 1)]

    far = chip_at((pos + hops) % chips, chips)
    wide_depth = 2 * depth
    half = rows // 2

    def term(which, g, columns, first):
        rows_here = pl.ds(pl.multiple_of(which * wide_depth, wide_depth), wide_depth)
        return jnp.dot(
            normed[which, first : first + half, :],
            w[g, rows_here, columns],
            preferred_element_type=jnp.float32,
        )

    def near(g, columns, first):
        total = bias[g, :, columns]
        for step in range(1, chips):
            total = total + term((far + step) % chips, g, columns, first)
        return total

    def start(g):
        landed(pair_recv.at[g], 2 * hops - 1)
        early[g] = near(g, slice(None), 0)

    marks = [(j + 1) * ng // row_chunks for j in range(row_chunks)]
    marks[-1] = ng
    ready = marks[row_chunks // 2 - 1]
    per_step = -(-ng // (ng - ready))
    for t in range(1, hops):
        done = 0
        for j, mark in enumerate(marks):

            @pl.loop(done, mark)
            def _(g):
                landed(ring_recv.at[t - 1, g], 2)
                for d in range(2):
                    here = slot(g, block_of(d, t, core))
                    if t + 1 < hops:
                        pass_on(here, ring_recv.at[t, g], towards[d])
                    else:
                        for k in range(SLOT):
                            c = g * SLOT + k
                            last = nh - 1 + d * nh

                            @pl.when((c < last) if d == 0 else ((c >= nh) & (c < last)))
                            def _():
                                pass_on(
                                    piece(c, block_of(d, t, core)),
                                    far_recv.at[c - d * nh],
                                    towards[d],
                                )

                            if k == last % SLOT:

                                @pl.when(c == last)
                                def _():
                                    for p in range(PARTS):
                                        pltpu.make_async_remote_copy(
                                            src_ref=w.at[
                                                last // SLOT,
                                                half_of(block_of(d, t, core), p),
                                                pl.ds(k * CW + p // 2 * HALF, HALF),
                                            ],
                                            dst_ref=last_part(d, core, p),
                                            send_sem=pass_send,
                                            recv_sem=far_recv.at[nh - 1 + p],
                                            device_id={"rep": towards[d]},
                                            device_id_type=MESH,
                                        ).start()

                    pass_on(here, pair_recv.at[g], partner)
                if t + 1 == hops and (t > 1 or done >= ready):
                    for k in range(per_step):
                        other = (g - ready) * per_step + k

                        @pl.when(jnp.logical_and(other >= 0, other < ng))
                        def _():
                            start(other)

            done = mark
            if t == 1:
                rebuild(j)

    def partial(i):
        for d in range(2):
            c = i + d * nh
            sums[i % 2, d] = near(c // SLOT, columns_of(c), half)

    def finish(i):
        for d in range(2):
            c = i + d * nh
            for first in (0, half):
                if first == 0:
                    total = early[c // SLOT, :, columns_of(c)]
                else:
                    total = sums[i % 2, d]
                total = total + term(far, c // SLOT, columns_of(c), first)
                result = total.astype(jnp.bfloat16)
                here = slice(first, first + half)

                @pl.when(c < nq)
                def _():
                    q_ref[0, here, pl.ds(pl.multiple_of(c * CW, CW), CW)] = result

                @pl.when(c >= nq)
                def _():
                    kv_ref[0, here, pl.ds(pl.multiple_of((c - nq) * CW, CW), CW)] = result

    def arrived(i):
        landed(far_recv.at[i], 2, CW)
        for d in range(2):
            pass_on(piece(i + d * nh, block_of(d, hops, core)), pair_recv.at[i], partner)

    partial(0)
    last_normed[...] = normed[far]
    for d in range(2):
        c = nh - 1 + d * nh
        columns = slice((c % SLOT) * CW, (c % SLOT + 1) * CW)
        last_sums[d, :half, :] = early[c // SLOT, :, columns]
        last_sums[d, half:, :] = near(c // SLOT, columns, half)

    @pl.loop(0, nh - 1)
    def _(i):
        arrived(i)

        @pl.when(i + 1 < nh - 1)
        def _():
            partial(i + 1)

        landed(pair_recv.at[i], 2, CW)
        finish(i)

    for p in range(PARTS):
        landed(far_recv.at[nh - 1 + p], 1, HALF)
        for d in range(2):
            pass_on(last_part(d, core, p), pair_recv.at[nh - 1 + p], partner)

    landed(own_send, 3, slots=ng)

    @pl.when(section < sections - 1)
    def _():
        for i in range(len(lists)):
            list_copy(i).wait_send()
        pltpu.make_async_copy(values, values, row_send).wait()

    landed(pass_send, 4 * hops - 4, slots=ng)
    for p in range(PARTS):
        landed(pair_recv.at[nh - 1 + p], 1, HALF)


def put_out(
    parts,
    rebuilt_ref,
    q_ref,
    kv_ref,
    last_w,
    last_normed,
    last_sums,
    rebuilt_out,
    q_out,
    kv_out,
    last,
    sem,
):
    rows = q_ref.shape[1]
    nq = q_ref.shape[2] // CW
    nc = nq + kv_ref.shape[2] // CW
    last_pieces = (nc // 2 - 1, nc - 1)

    step = rows // parts

    def out(source, target, base, k):
        count = source.shape[2] // CW
        cuts = [c - base for c in last_pieces if base <= c < base + count]
        for first, stop in zip([0] + [c + 1 for c in cuts], cuts + [count]):
            if first < stop:
                columns = pl.ds(first * CW, (stop - first) * CW)
                for j in range(parts):
                    here = pl.ds(j * step, step)
                    pltpu.make_async_copy(
                        source.at[:, here, columns], target.at[:, here, columns], sem.at[k]
                    ).start()
        whole = source.at[:, :, pl.ds(0, (count - len(cuts)) * CW)]
        return pltpu.make_async_copy(whole, whole, sem.at[k])

    arrays = ((rebuilt_ref, rebuilt_out, nc), (q_ref, q_out, 0), (kv_ref, kv_out, nq))
    waits = [out(source, target, base, k) for k, (source, target, base) in enumerate(arrays)]
    for d, c in enumerate(last_pieces):
        total = last_sums[d] + jnp.dot(
            last_normed[...], last_w[d], preferred_element_type=jnp.float32
        )
        last[d] = total.astype(jnp.bfloat16)
        target, base = (q_out, 0) if c < nq else (kv_out, nq)
        pltpu.make_async_copy(
            last.at[d], target.at[0, :, pl.ds((c - base) * CW, CW)], sem.at[len(arrays)]
        ).start()
    for copy in waits:
        copy.wait()
    pltpu.make_async_copy(last, last, sem.at[len(arrays)]).wait()


def body(
    cache,
    payload,
    block_ids,
    block_counts,
    block_scales,
    refresh_ids,
    refresh_counts,
    norm_gain,
    query_weight,
    query_bias,
    kv_weight,
    kv_bias,
):
    sections = lax.axis_size("section")
    reps = lax.axis_size("rep")
    rows, feature = cache.shape[1:]
    depth = query_weight.shape[1]
    queries = query_weight.shape[2]
    keys = kv_weight.shape[2]
    most_blk = block_ids.shape[2]
    ng = (queries + keys) // GW
    nh = ng * SLOT // 2
    hops = reps // 4
    row_chunks = rows // BLK

    lists = (refresh_ids[0], block_ids[0], block_scales[0], block_counts, refresh_counts)
    vmem = pl.BlockSpec(memory_space=pltpu.VMEM)
    anywhere = pl.BlockSpec(memory_space=pltpu.HBM)
    dma = pltpu.SemaphoreType.DMA
    results = pl.pallas_call(
        functools.partial(kernel, sections, reps, most_blk),
        out_shape=(
            pltpu.VMEM(cache.shape, cache.dtype),
            pltpu.VMEM((1, rows, queries), cache.dtype),
            pltpu.VMEM((1, rows, keys), cache.dtype),
            pltpu.VMEM((2, 2 * depth, CW), jnp.bfloat16),
            pltpu.VMEM((rows, 2 * depth), jnp.bfloat16),
            pltpu.VMEM((2, rows, CW), jnp.float32),
        ),
        in_specs=[(anywhere,) * len(lists)] + [anywhere] * 7,
        out_specs=(vmem,) * 6,
        scratch_shapes=[
            pltpu.VMEM((ng, reps * depth, GW), jnp.bfloat16),
            pltpu.VMEM((reps // 2, rows, 2 * depth), jnp.bfloat16),
            pltpu.VMEM((ng, rows // 2, GW), jnp.float32),
            pltpu.VMEM((2, 2, rows // 2, CW), jnp.float32),
            pltpu.VMEM((rows, feature), jnp.bfloat16),
            pltpu.VMEM(norm_gain.shape, jnp.float32),
            pltpu.VMEM((ng, 1, GW), jnp.float32),
            tuple(pltpu.VMEM(x.shape, x.dtype) for x in lists),
            dma((2,)),
            dma,
            dma((2,)),
            dma,
            dma((row_chunks,)),
            dma((len(lists),)),
            dma((len(lists),)),
            dma,
            dma,
            dma((hops - 1, ng)),
            dma((max(ng, nh - 1 + PARTS),)),
            dma((nh - 1 + PARTS,)),
        ],
        compiler_params=pltpu.CompilerParams(
            collective_id=0, has_side_effects=True, vmem_limit_bytes=KERNEL_VMEM
        ),
    )(lists, payload, cache, norm_gain, query_weight, query_bias, kv_weight, kv_bias)
    return tuple(
        pl.pallas_call(
            functools.partial(put_out, 2),
            out_shape=tuple(pltpu.HBM(x.shape, x.dtype) for x in results[:3]),
            in_specs=[vmem] * len(results),
            out_specs=(anywhere,) * 3,
            scratch_shapes=[
                pltpu.VMEM((2, rows, CW), jnp.bfloat16),
                dma((4,)),
            ],
            compiler_params=pltpu.CompilerParams(vmem_limit_bytes=OUT_VMEM),
        )(*results)
    )


def solution(mesh):
    in_specs = (
        P("section", "rep", None),
        P("section", "rep", None),
        P("section", "rep", None),
        P("section", "rep"),
        P("section", "rep", None),
        P("section", "rep", None),
        P("section", "rep"),
        P("section", None),
        P("section", "rep", None),
        P("section", None),
        P("section", "rep", None),
        P("section", None),
    )
    out_specs = (P("section", "rep", None), P("section", "rep", None), P("section", "rep", None))
    return jax.shard_map(body, mesh=mesh, in_specs=in_specs, out_specs=out_specs, check_vma=False)
```

```python
import functools

import jax
import jax.numpy as jnp
from jax import lax
from jax.experimental import pallas as pl
from jax.experimental.pallas import tpu as pltpu
from jax.sharding import PartitionSpec as P

BLK = 128
HALF = 128
CW = 256
PARTS = 2 * CW // HALF
SLOT = 2
GW = SLOT * CW
TILE = 16
EPSILON = 1e-06
KERNEL_VMEM = 100 * 512 * 1024
OUT_VMEM = 3 * 1024 * 1024
MESH = pl.DeviceIdType.MESH


def chip_at(pos, chips):
    half = chips // 2
    back = pos // half
    return pos + back * (half + chips - 1 - 2 * pos)


def kernel(
    sections,
    reps,
    most_blk,
    lists_ref,
    payload_ref,
    cache_ref,
    gain_hbm,
    qw_ref,
    qb_hbm,
    kvw_ref,
    kvb_hbm,
    rebuilt_ref,
    q_ref,
    kv_ref,
    last_w,
    last_normed,
    last_sums,
    w,
    normed,
    early,
    sums,
    values,
    gain_ref,
    bias,
    lists,
    local_sem,
    keep_sem,
    small_sem,
    row_send,
    row_recv,
    list_send,
    list_recv,
    own_send,
    pass_send,
    ring_recv,
    pair_recv,
    far_recv,
):
    chips = reps // 2
    hops = chips // 2
    depth = qw_ref.shape[1]
    rows = payload_ref.shape[1]
    feature = payload_ref.shape[2]
    ngq = qw_ref.shape[2] // GW
    ng = ngq + kvw_ref.shape[2] // GW
    nq = ngq * SLOT
    nc = ng * SLOT
    nh = nc // 2
    row_chunks = rows // BLK

    section = lax.axis_index("section")
    me = lax.axis_index("rep")
    core = me % 2
    chip = me // 2
    pos = chip + (chip // hops) * (hops + chips - 1 - 2 * chip)
    partner = 2 * chip + (1 - core)

    def rep_at(place, which):
        return 2 * chip_at((place + chips) % chips, chips) + which

    towards = (rep_at(pos + 1, core), rep_at(pos - 1, core))

    barrier = pltpu.get_barrier_semaphore()
    for other in towards + (partner,):
        pl.semaphore_signal(barrier, 1, device_id={"rep": other}, device_id_type=MESH)

    @pl.when(section > 0)
    def _():
        pl.semaphore_signal(
            barrier, 1, device_id={"section": section - 1}, device_id_type=MESH
        )

    @pl.when(section < sections - 1)
    def _():
        pl.semaphore_signal(
            barrier, 1, device_id={"section": section + 1}, device_id_type=MESH
        )

    def own(g):
        if g < ngq:
            return qw_ref.at[0, :, pl.ds(g * GW, GW)]
        return kvw_ref.at[0, :, pl.ds((g - ngq) * GW, GW)]

    def depth_of(block):
        return pl.ds(pl.multiple_of(block * depth, depth), depth)

    def columns_of(c):
        return pl.ds(pl.multiple_of((c % SLOT) * CW, CW), CW)

    def slot(g, block):
        return w.at[g, depth_of(block), :]

    def piece(c, block):
        return w.at[c // SLOT, depth_of(block), columns_of(c)]

    def half_of(block, p):
        first = block * depth + p % 2 * (depth // 2)
        return pl.ds(pl.multiple_of(first, depth // 2), depth // 2)

    def last_part(d, which, p):
        return last_w.at[d, half_of(which, p), pl.ds(p // 2 * HALF, HALF)]

    keep = pltpu.make_async_copy(cache_ref, rebuilt_ref, keep_sem)
    gain_copy = pltpu.make_async_copy(gain_hbm, gain_ref, small_sem.at[0])
    small = [gain_copy]
    for g in range(ng):
        source, first = (qb_hbm, g) if g < ngq else (kvb_hbm, g - ngq)
        small.append(
            pltpu.make_async_copy(source.at[:, pl.ds(first * GW, GW)], bias.at[g], small_sem.at[1])
        )
    own_locals = [
        pltpu.make_async_copy(own(g), slot(g, me), local_sem.at[min(g, 1)]) for g in range(ng)
    ]

    sides = (section + sections - 1) // sections + (2 * sections - 2 - section) // sections
    own_locals[0].start()
    pl.semaphore_wait(barrier, 3 + sides)
    own_locals[0].wait()

    def list_copy(i):
        return pltpu.make_async_remote_copy(
            src_ref=lists_ref[i],
            dst_ref=lists[i],
            send_sem=list_send.at[i],
            recv_sem=list_recv.at[i],
            device_id={"section": section + 1},
            device_id_type=MESH,
        )

    def row_copy(j):
        return pltpu.make_async_remote_copy(
            src_ref=payload_ref.at[0, pl.ds(j * BLK, BLK), :],
            dst_ref=values.at[pl.ds(j * BLK, BLK), :],
            send_sem=row_send,
            recv_sem=row_recv.at[j],
            device_id={"section": section + 1},
            device_id_type=MESH,
        )

    for g in range(ng):
        source = own(g) if g else slot(g, me)
        for d in range(2):
            pltpu.make_async_remote_copy(
                src_ref=source,
                dst_ref=slot(g, me),
                send_sem=own_send,
                recv_sem=ring_recv.at[0, g],
                device_id={"rep": towards[d]},
                device_id_type=MESH,
            ).start()
        if g == 0:

            @pl.when(section < sections - 1)
            def _():
                for j in range(row_chunks):
                    row_copy(j).start()
                    if j == 0:
                        for i in range(len(lists)):
                            list_copy(i).start()

            keep.start()
            for copy in small:
                copy.start()

        pltpu.make_async_remote_copy(
            src_ref=source,
            dst_ref=slot(g, me),
            send_sem=own_send,
            recv_sem=pair_recv.at[g],
            device_id={"rep": partner},
            device_id_type=MESH,
        ).start()
        if g:
            own_locals[g].start()

    @pl.when(section == 0)
    def _():
        for ref in lists:
            ref[...] = jnp.zeros_like(ref)

        @pl.loop(0, rows // TILE)
        def _(i):
            values[pl.ds(i * TILE, TILE), :] = jnp.zeros((TILE, feature), values.dtype)

    def landed(sem, blocks, width=GW, slots=1):
        part = w.at[pl.ds(0, slots), pl.ds(0, blocks * depth), pl.ds(0, width)]
        pltpu.make_async_copy(part, part, sem).wait()

    gain_copy.wait()
    pltpu.make_async_copy(bias, bias, small_sem.at[1]).wait()
    keep.wait()
    landed(local_sem.at[1], 1, slots=ng - 1)

    def block_of(d, t, which):
        return rep_at(pos - t if d == 0 else pos + t, which)

    def pass_on(here, recv_sem, target):
        pltpu.make_async_remote_copy(
            src_ref=here,
            dst_ref=here,
            send_sem=pass_send,
            recv_sem=recv_sem,
            device_id={"rep": target},
            device_id_type=MESH,
        ).start()

    def rebuild(j):
        @pl.when(section > 0)
        def _():
            if j == 0:
                for i in range(len(lists)):
                    list_copy(i).wait_recv()
            row_copy(j).wait_recv()

        got_rows, got_ids, got_scales, got_counts, got_rcounts = lists
        count = got_counts[...]
        factor = jnp.zeros((1, 1), jnp.float32)
        for i in range(most_blk):
            live = jnp.logical_and(got_ids[:, i : i + 1] == j, count > i)
            scale = got_scales[:, i : i + 1].astype(jnp.float32) / 4096.0
            factor = factor + jnp.where(live, scale, 0.0)

        @pl.loop(0, BLK // TILE)
        def _(i):
            first = j * BLK + i * TILE
            here = pl.ds(pl.multiple_of(first, TILE), TILE)
            ids = got_rows[...]
            lanes = lax.broadcasted_iota(jnp.int32, ids.shape, 1)
            ids = jnp.where(lanes < got_rcounts[...], ids, -1)
            number = first + lax.broadcasted_iota(jnp.int32, (TILE, ids.shape[1]), 0)
            match = jnp.where(ids == number, 1.0, 0.0)
            hit = jnp.max(match, axis=1, keepdims=True) > 0.0
            got = values[here, :].astype(jnp.float32)
            delta = (got * factor).astype(jnp.bfloat16).astype(jnp.float32)
            mixed = jnp.where(hit, got, rebuilt_ref[0, here, :].astype(jnp.float32) + delta)
            rebuilt = mixed.astype(jnp.bfloat16)
            rebuilt_ref[0, here, :] = rebuilt
            wide = rebuilt.astype(jnp.float32)
            mean = jnp.sum(wide * wide, axis=1, keepdims=True) / feature
            scale_rows = lax.rsqrt(mean + EPSILON)
            result = (wide * scale_rows * gain_ref[...]).astype(jnp.bfloat16)
            for k in range(chips):
                normed[k, here, :] = result[:, 2 * depth * k : 2 * depth * (k + 1)]

    far = chip_at((pos + hops) % chips, chips)
    wide_depth = 2 * depth
    half = rows // 2

    def term(which, g, columns, first):
        rows_here = pl.ds(pl.multiple_of(which * wide_depth, wide_depth), wide_depth)
        return jnp.dot(
            normed[which, first : first + half, :],
            w[g, rows_here, columns],
            preferred_element_type=jnp.float32,
        )

    def near(g, columns, first):
        total = bias[g, :, columns]
        for step in range(1, chips):
            total = total + term((far + step) % chips, g, columns, first)
        return total

    def start(g):
        landed(pair_recv.at[g], 2 * hops - 1)
        early[g] = near(g, slice(None), 0)

    marks = [(j + 1) * ng // row_chunks for j in range(row_chunks)]
    marks[-1] = ng
    ready = marks[row_chunks // 2 - 1]
    per_step = -(-ng // (ng - ready))
    for t in range(1, hops):
        done = 0
        for j, mark in enumerate(marks):

            @pl.loop(done, mark)
            def _(g):
                landed(ring_recv.at[t - 1, g], 2)
                for d in range(2):
                    here = slot(g, block_of(d, t, core))
                    if t + 1 < hops:
                        pass_on(here, ring_recv.at[t, g], towards[d])
                    else:
                        for k in range(SLOT):
                            c = g * SLOT + k
                            last = nh - 1 + d * nh

                            @pl.when((c < last) if d == 0 else ((c >= nh) & (c < last)))
                            def _():
                                pass_on(
                                    piece(c, block_of(d, t, core)),
                                    far_recv.at[c - d * nh],
                                    towards[d],
                                )

                            if k == last % SLOT:

                                @pl.when(c == last)
                                def _():
                                    for p in range(PARTS):
                                        pltpu.make_async_remote_copy(
                                            src_ref=w.at[
                                                last // SLOT,
                                                half_of(block_of(d, t, core), p),
                                                pl.ds(k * CW + p // 2 * HALF, HALF),
                                            ],
                                            dst_ref=last_part(d, core, p),
                                            send_sem=pass_send,
                                            recv_sem=far_recv.at[nh - 1 + p],
                                            device_id={"rep": towards[d]},
                                            device_id_type=MESH,
                                        ).start()

                    pass_on(here, pair_recv.at[g], partner)
                if t + 1 == hops and (t > 1 or done >= ready):
                    for k in range(per_step):
                        other = (g - ready) * per_step + k

                        @pl.when(jnp.logical_and(other >= 0, other < ng))
                        def _():
                            start(other)

            done = mark
            if t == 1:
                rebuild(j)

    def partial(i):
        for d in range(2):
            c = i + d * nh
            sums[i % 2, d] = near(c // SLOT, columns_of(c), half)

    def finish(i):
        for d in range(2):
            c = i + d * nh
            for first in (0, half):
                if first == 0:
                    total = early[c // SLOT, :, columns_of(c)]
                else:
                    total = sums[i % 2, d]
                total = total + term(far, c // SLOT, columns_of(c), first)
                result = total.astype(jnp.bfloat16)
                here = slice(first, first + half)

                @pl.when(jnp.asarray(c < nq))
                def _():
                    q_ref[0, here, pl.ds(pl.multiple_of(c * CW, CW), CW)] = result

                @pl.when(jnp.asarray(c >= nq))
                def _():
                    kv_ref[0, here, pl.ds(pl.multiple_of((c - nq) * CW, CW), CW)] = result

    def arrived(i):
        landed(far_recv.at[i], 2, CW)
        for d in range(2):
            pass_on(piece(i + d * nh, block_of(d, hops, core)), pair_recv.at[i], partner)

    partial(0)
    last_normed[...] = normed[far]
    for d in range(2):
        c = nh - 1 + d * nh
        columns = slice((c % SLOT) * CW, (c % SLOT + 1) * CW)
        last_sums[d, :half, :] = early[c // SLOT, :, columns]
        last_sums[d, half:, :] = near(c // SLOT, columns, half)

    @pl.loop(0, nh - 2)
    def _(i):
        arrived(i)

        @pl.when(i + 1 < nh - 1)
        def _():
            partial(i + 1)

        landed(pair_recv.at[i], 2, CW)
        finish(i)

    arrived(nh - 2)

    def pass_last():
        for p in range(PARTS):
            landed(far_recv.at[nh - 1 + p], 1, HALF)
            for d in range(2):
                pass_on(last_part(d, core, p), pair_recv.at[nh - 1 + p], partner)

    @pl.when(core == 1)
    def _():
        pass_last()

    landed(pair_recv.at[nh - 2], 2, CW)
    finish(nh - 2)

    @pl.when(core == 0)
    def _():
        pass_last()

    landed(own_send, 3, slots=ng)

    @pl.when(section < sections - 1)
    def _():
        for i in range(len(lists)):
            list_copy(i).wait_send()
        pltpu.make_async_copy(values, values, row_send).wait()

    landed(pass_send, 4 * hops - 4, slots=ng)
    for p in range(PARTS):
        landed(pair_recv.at[nh - 1 + p], 1, HALF)


def put_out(
    parts,
    rebuilt_ref,
    q_ref,
    kv_ref,
    last_w,
    last_normed,
    last_sums,
    rebuilt_out,
    q_out,
    kv_out,
    last,
    sem,
):
    rows = q_ref.shape[1]
    nq = q_ref.shape[2] // CW
    nc = nq + kv_ref.shape[2] // CW
    last_pieces = (nc // 2 - 1, nc - 1)

    step = rows // parts

    def out(source, target, base, k):
        count = source.shape[2] // CW
        cuts = [c - base for c in last_pieces if base <= c < base + count]
        for first, stop in zip([0] + [c + 1 for c in cuts], cuts + [count]):
            if first < stop:
                columns = pl.ds(first * CW, (stop - first) * CW)
                for j in range(parts):
                    here = pl.ds(j * step, step)
                    pltpu.make_async_copy(
                        source.at[:, here, columns], target.at[:, here, columns], sem.at[k]
                    ).start()
        whole = source.at[:, :, pl.ds(0, (count - len(cuts)) * CW)]
        return pltpu.make_async_copy(whole, whole, sem.at[k])

    arrays = ((rebuilt_ref, rebuilt_out, nc), (q_ref, q_out, 0), (kv_ref, kv_out, nq))
    waits = [out(source, target, base, k) for k, (source, target, base) in enumerate(arrays)]
    for d, c in enumerate(last_pieces):
        total = last_sums[d] + jnp.dot(
            last_normed[...], last_w[d], preferred_element_type=jnp.float32
        )
        last[d] = total.astype(jnp.bfloat16)
        target, base = (q_out, 0) if c < nq else (kv_out, nq)
        pltpu.make_async_copy(
            last.at[d], target.at[0, :, pl.ds((c - base) * CW, CW)], sem.at[len(arrays)]
        ).start()
    for copy in waits:
        copy.wait()
    pltpu.make_async_copy(last, last, sem.at[len(arrays)]).wait()


def body(
    cache,
    payload,
    block_ids,
    block_counts,
    block_scales,
    refresh_ids,
    refresh_counts,
    norm_gain,
    query_weight,
    query_bias,
    kv_weight,
    kv_bias,
):
    sections = lax.axis_size("section")
    reps = lax.axis_size("rep")
    rows, feature = cache.shape[1:]
    depth = query_weight.shape[1]
    queries = query_weight.shape[2]
    keys = kv_weight.shape[2]
    most_blk = block_ids.shape[2]
    ng = (queries + keys) // GW
    nh = ng * SLOT // 2
    hops = reps // 4
    row_chunks = rows // BLK

    lists = (refresh_ids[0], block_ids[0], block_scales[0], block_counts, refresh_counts)
    vmem = pl.BlockSpec(memory_space=pltpu.VMEM)
    anywhere = pl.BlockSpec(memory_space=pltpu.HBM)
    dma = pltpu.SemaphoreType.DMA
    results = pl.pallas_call(
        functools.partial(kernel, sections, reps, most_blk),
        out_shape=(
            pltpu.VMEM(cache.shape, cache.dtype),
            pltpu.VMEM((1, rows, queries), cache.dtype),
            pltpu.VMEM((1, rows, keys), cache.dtype),
            pltpu.VMEM((2, 2 * depth, CW), jnp.bfloat16),
            pltpu.VMEM((rows, 2 * depth), jnp.bfloat16),
            pltpu.VMEM((2, rows, CW), jnp.float32),
        ),
        in_specs=[(anywhere,) * len(lists)] + [anywhere] * 7,
        out_specs=(vmem,) * 6,
        scratch_shapes=[
            pltpu.VMEM((ng, reps * depth, GW), jnp.bfloat16),
            pltpu.VMEM((reps // 2, rows, 2 * depth), jnp.bfloat16),
            pltpu.VMEM((ng, rows // 2, GW), jnp.float32),
            pltpu.VMEM((2, 2, rows // 2, CW), jnp.float32),
            pltpu.VMEM((rows, feature), jnp.bfloat16),
            pltpu.VMEM(norm_gain.shape, jnp.float32),
            pltpu.VMEM((ng, 1, GW), jnp.float32),
            tuple(pltpu.VMEM(x.shape, x.dtype) for x in lists),
            dma((2,)),
            dma,
            dma((2,)),
            dma,
            dma((row_chunks,)),
            dma((len(lists),)),
            dma((len(lists),)),
            dma,
            dma,
            dma((hops - 1, ng)),
            dma((max(ng, nh - 1 + PARTS),)),
            dma((nh - 1 + PARTS,)),
        ],
        compiler_params=pltpu.CompilerParams(
            collective_id=0, has_side_effects=True, vmem_limit_bytes=KERNEL_VMEM
        ),
    )(lists, payload, cache, norm_gain, query_weight, query_bias, kv_weight, kv_bias)
    return tuple(
        pl.pallas_call(
            functools.partial(put_out, 2),
            out_shape=tuple(pltpu.HBM(x.shape, x.dtype) for x in results[:3]),
            in_specs=[vmem] * len(results),
            out_specs=(anywhere,) * 3,
            scratch_shapes=[
                pltpu.VMEM((2, rows, CW), jnp.bfloat16),
                dma((4,)),
            ],
            compiler_params=pltpu.CompilerParams(vmem_limit_bytes=OUT_VMEM),
        )(*results)
    )


def solution(mesh):
    in_specs = (
        P("section", "rep", None),
        P("section", "rep", None),
        P("section", "rep", None),
        P("section", "rep"),
        P("section", "rep", None),
        P("section", "rep", None),
        P("section", "rep"),
        P("section", None),
        P("section", "rep", None),
        P("section", None),
        P("section", "rep", None),
        P("section", None),
    )
    out_specs = (P("section", "rep", None), P("section", "rep", None), P("section", "rep", None))
    return jax.shard_map(body, mesh=mesh, in_specs=in_specs, out_specs=out_specs, check_vma=False)
```
